32 devices in a mesh: grp: 4 (over z), dev: 8 (over y, x, core).
Axes of the slice: x: 2, y: 2, z: 4, core: 2. Of those that a mesh axis runs over, the one named last changes fastest.
Arguments:
- matrix_tiles: bfloat16 [640, 128, 1024], P(('grp', 'dev')), may hold values from -0.125 to 0.125
- tile_column: int32 [640], P(('grp', 'dev')), may hold values from 0 to 255
- block_counts: int32 [256], P(('grp', 'dev')), may hold values from 1 to 4, as said below
- destination: int32 [256], P(('grp', 'dev')), may hold values from 0 to 7, as said below
- row_bounds: bfloat16 [32768], P(('grp', 'dev')), may hold values from -6 to 6
- dual_start: bfloat16 [32768], P(('grp', 'dev')), may hold values from 0 to 1
- primal_start: float32 [262144], replicated, may hold values from 0 to 0.5
- cost_vector: float32 [262144], replicated, may hold values from -6 to 6
- upper_bound: float32 [262144], replicated, may hold values from 0.5 to 2
Outputs:
- primal_final: float32 [262144], replicated
- dual_final: float32 [32768], P(('grp', 'dev'))
- weight_final: float32 [1], replicated
The draws below stay inside these ranges and needn't reach their ends.
Inputs may be any that keep to these rules, and one draw needn't show every extreme that they name: `block_counts`: each device's 8 row blocks have 1 to 4 tiles each and 20 at most together; some device has exactly 20 in every draw. `destination`: on every device the 8 entries are each of 0 to 7 once.
All inputs are finite; a program needn't handle non-finite values.
Results may differ from the reference program's by a relative error of at most 0.0015.
Values may be sent and summed in bfloat16 or wider, within the bound.
A program may use at most 128 MiB of HBM per device.

```python
import jax
import jax.numpy as jnp
from jax import lax

CB = 1024
NCB = 256
TR = 128
MAXC = 4
ITERS = 3
RB_DEV = 8
POOL_DEV = 20
RBLK = 256
ROWS = 32768
COLS = 262144
N_GRP = 4
N_DEV = 8


def layout_pair(key):
    device_count = RBLK // RB_DEV
    base_key = jax.random.fold_in(key, 7)
    key_extra, key_heavy, key_rank, key_tie = jax.random.split(base_key, 4)
    extra_tiles = jax.random.randint(key_extra, (device_count,), 0, POOL_DEV - RB_DEV + 1)
    heaviest = jax.random.randint(key_heavy, (), 0, device_count)
    extra_tiles = jnp.where(jnp.arange(device_count) == heaviest, POOL_DEV - RB_DEV, extra_tiles)
    rank_of = jax.vmap(lambda sub: jax.random.permutation(sub, RB_DEV))(jax.random.split(key_rank, device_count))
    counts = 1 + jnp.clip(extra_tiles[:, None] - rank_of * (MAXC - 1), 0, MAXC - 1)
    tie_break = jax.vmap(lambda sub: jax.random.permutation(sub, RB_DEV))(jax.random.split(key_tie, device_count))
    sorted_slots = jnp.argsort(counts * RB_DEV + tie_break, axis=1)
    position = jnp.argsort(sorted_slots, axis=1)
    member = (jnp.arange(device_count) % RB_DEV)[:, None]
    target_dev = (position + member) % RB_DEV
    return (counts.astype(jnp.int32).reshape(RBLK), target_dev.astype(jnp.int32).reshape(RBLK))


def draw_block_counts(key, part):
    return layout_pair(key)[0]


def draw_destination(key, part):
    return layout_pair(key)[1]


def plant(result, rng, low, top_value):
    longest = result.shape.index(max(result.shape))
    spots = []
    for shift in (0, 1):
        where = [jax.random.randint(jax.random.fold_in(rng, axis), (), 0, length) for axis, length in enumerate(result.shape)]
        where[longest] = (where[longest] + shift) % result.shape[longest]
        spots.append(tuple(where))
    return result.at[spots[0]].set(low).at[spots[1]].set(top_value)


def steps_of(own_key, extent, shards, low, top_value):
    level = 1.0
    for dim, blocks in shards:
        heights = jax.random.uniform(jax.random.fold_in(jax.random.fold_in(own_key, 6), dim), (blocks,), jnp.float32, low / len(shards), top_value / len(shards))
        level = level * jnp.repeat(jnp.exp(heights), extent[dim] // blocks).reshape((-1,) + (1,) * (len(extent) - 1 - dim))
    return level


def bell_draw(own_key, shape, spread, reach, cuts=(), kind=jnp.bfloat16):
    gain = steps_of(own_key, shape, cuts, -0.22, 0.18) if cuts else 1.0
    drawn = jax.random.normal(own_key, shape, jnp.float32) * spread * gain
    return jnp.minimum(jnp.maximum(drawn, -reach), reach).astype(kind)


def setup_inputs(seed: int = 0) -> dict:
    key_list = jax.random.split(jax.random.key(seed), 10)
    matrix_tiles = bell_draw(key_list[0], (N_GRP * N_DEV * POOL_DEV, TR, CB), (2 * CB) ** -0.5, 0.125, ((0, 32),))
    tile_column = plant(jax.random.randint(key_list[1], (N_GRP * N_DEV * POOL_DEV,), 0, NCB), jax.random.fold_in(key_list[1], 1), 0, NCB - 1).astype(jnp.int32)
    block_counts = draw_block_counts(jax.random.fold_in(key_list[9], 71), 0)
    destination = draw_destination(jax.random.fold_in(key_list[9], 71), 0)
    row_bounds = bell_draw(key_list[4], (ROWS,), 1.0, 6.0, ((0, 32),))
    dual_start = jnp.clip(1.0 * jax.random.uniform(key_list[5], (ROWS,), jnp.float32) ** steps_of(key_list[5], (ROWS,), ((0, 32),), -0.2, 0.2), 0.0, 1.0).astype(jnp.bfloat16)
    primal_start = jnp.clip(jax.random.uniform(key_list[6], (COLS,), jnp.float32, 0.0, 0.5), 0.0, 0.5)
    cost_vector = bell_draw(key_list[7], (COLS,), 1.0, 6.0, (), jnp.float32)
    upper_bound = jnp.clip(jax.random.uniform(key_list[8], (COLS,), jnp.float32, 0.5, 2.0), 0.5, 2.0)
    return {"matrix_tiles": matrix_tiles, "tile_column": tile_column, "block_counts": block_counts, "destination": destination, "row_bounds": row_bounds, "dual_start": dual_start, "primal_start": primal_start, "cost_vector": cost_vector, "upper_bound": upper_bound}


step_scale = 0.3

def reference(matrix_tiles, tile_column, block_counts, destination, row_bounds, dual_start, primal_start, cost_vector, upper_bound):
    device_count = N_GRP * N_DEV
    tile_set = matrix_tiles.reshape(device_count, POOL_DEV, TR, CB)
    tile_cols = tile_column.reshape(device_count, POOL_DEV)
    counts = block_counts.reshape(device_count, RB_DEV)
    starts = jnp.cumsum(counts, axis=1) - counts
    slot_ids = jnp.arange(POOL_DEV, dtype=jnp.int32)
    owners = lax.optimization_barrier(jnp.sum((starts[:, None, 1:] <= slot_ids[None, :, None]).astype(jnp.int32), axis=2))
    is_live = slot_ids[None, :] < lax.optimization_barrier(jnp.sum(counts, axis=1))[:, None]

    def apply_rows(vector_bf):
        vector_table = vector_bf.astype(jnp.float32).reshape(NCB, CB)

        def per_device(entries):
            tile_d, col_d, own_d, live_d = entries
            product = jnp.einsum('src,sc->sr', tile_d.astype(jnp.float32), vector_table[col_d], precision=lax.Precision.HIGHEST)
            product = jnp.where(live_d[:, None], product, 0.0)
            return jax.ops.segment_sum(product, own_d, num_segments=RB_DEV)
        return lax.map(per_device, (tile_set, tile_cols, owners, is_live))

    def apply_columns(rows_bf):

        def per_device(accum, entries):
            tile_d, col_d, own_d, live_d, rows_d = entries
            product = jnp.einsum('src,sr->sc', tile_d.astype(jnp.float32), rows_d.astype(jnp.float32)[own_d], precision=lax.Precision.HIGHEST)
            product = jnp.where(live_d[:, None], product, 0.0)
            return (accum + jax.ops.segment_sum(product, col_d, num_segments=NCB), None)
        accum, unused = lax.scan(per_device, jnp.zeros((NCB, CB), jnp.float32), (tile_set, tile_cols, owners, is_live, rows_bf))
        return accum.reshape(-1)
    bounds = row_bounds.astype(jnp.float32).reshape(device_count, RB_DEV, TR)
    dual_state = dual_start.astype(jnp.float32).reshape(device_count, RB_DEV, TR)
    primal = primal_start
    weight = jnp.ones((), jnp.float32)
    row_image = apply_rows(primal.astype(jnp.bfloat16))
    for iteration in range(ITERS):
        step_primal = step_scale / weight
        step_dual = step_scale * weight
        gradient = apply_columns(dual_state.astype(jnp.bfloat16))
        primal_next = jnp.clip(primal - step_primal * (cost_vector - gradient), 0.0, upper_bound)
        change = jnp.sum((primal_next - primal) ** 2)
        next_image = apply_rows(primal_next.astype(jnp.bfloat16))
        dual_state = jnp.maximum(dual_state + step_dual * (bounds - (2.0 * next_image - row_image)), 0.0)
        violation = jnp.sum(jnp.maximum(bounds - next_image, 0.0) ** 2)
        weight = jnp.sqrt(weight * jnp.sqrt((violation + 1e-06) / (change + 1e-06)))
        primal = primal_next
        row_image = next_image
    grouped = dual_state.reshape(N_GRP, N_DEV, RB_DEV, TR)
    target = destination.reshape(N_GRP, N_DEV, RB_DEV)
    group_index = jnp.broadcast_to(jnp.arange(N_GRP, dtype=jnp.int32)[:, None, None], target.shape)
    member_index = jnp.broadcast_to(jnp.arange(N_DEV, dtype=jnp.int32)[None, :, None], target.shape)
    placed = jnp.zeros((N_GRP, N_DEV, N_DEV, TR), jnp.float32).at[group_index, target, member_index].set(grouped)
    return (primal, placed.reshape(-1), jnp.reshape(weight, (1,)))
```

```python
import functools

import jax
import jax.numpy as jnp
from jax import lax
from jax.experimental import pallas as pl
from jax.experimental.pallas import tpu as pltpu
from jax.sharding import PartitionSpec as P

NCB = 256
ITERS = 3


step_scale = 0.3


def row_products(tile_store, vector_bf, blocks):
    tile_set, tile_cols, owners, live_flags = tile_store
    vector_table = vector_bf.reshape(-1, tile_set.shape[2])
    column_hot = (
        tile_cols[:, None] == jnp.arange(vector_table.shape[0], dtype=jnp.int32)[None, :]
    ).astype(jnp.bfloat16)
    picked = jnp.dot(column_hot, vector_table, preferred_element_type=jnp.float32).astype(
        jnp.bfloat16
    )
    product = jnp.einsum("src,sc->sr", tile_set, picked, preferred_element_type=jnp.float32)
    product = jnp.where(live_flags[:, None], product, 0.0)
    owner_hot = (jnp.arange(blocks, dtype=jnp.int32)[:, None] == owners[None, :]).astype(
        jnp.float32
    )
    return jnp.dot(owner_hot, product, precision=lax.Precision.HIGHEST)


def column_products(tile_store, rows_bf):
    tile_set, tile_cols, owners, live_flags = tile_store
    blocks = rows_bf.shape[0]
    owner_hot = (owners[:, None] == jnp.arange(blocks, dtype=jnp.int32)[None, :]).astype(
        jnp.bfloat16
    )
    picked_rows = jnp.dot(owner_hot, rows_bf, preferred_element_type=jnp.float32).astype(
        jnp.bfloat16
    )
    product = jnp.einsum("src,sr->sc", tile_set, picked_rows, preferred_element_type=jnp.float32)
    product = jnp.where(live_flags[:, None], product, 0.0)
    column_hot = (jnp.arange(NCB, dtype=jnp.int32)[:, None] == tile_cols[None, :]).astype(
        jnp.float32
    )
    return jnp.dot(column_hot, product, precision=lax.Precision.HIGHEST).reshape(-1)


def per_device(
    matrix_tiles,
    tile_column,
    block_counts,
    destination,
    row_bounds,
    dual_start,
    primal_start,
    cost_vector,
    upper_bound,
):
    blocks = block_counts.shape[0]
    rows_per = matrix_tiles.shape[1]
    slot_count = matrix_tiles.shape[0]
    starts = jnp.cumsum(block_counts) - block_counts
    slot_ids = jnp.arange(slot_count, dtype=jnp.int32)
    owners = jnp.sum((starts[None, 1:] <= slot_ids[:, None]).astype(jnp.int32), axis=1)
    bounds_here = row_bounds.reshape(blocks, rows_per)
    dual_here = dual_start.reshape(blocks, rows_per)
    peer_ids = jnp.arange(blocks, dtype=jnp.int32)
    inverse = jnp.sum(
        jnp.where(destination[None, :] == peer_ids[:, None], peer_ids[None, :], 0), axis=1
    )
    tile_store = (matrix_tiles, tile_column, owners, slot_ids < jnp.sum(block_counts))
    bounds = bounds_here.astype(jnp.float32)
    dual_state = dual_here.astype(jnp.float32)
    primal = primal_start
    weight = jnp.ones((), jnp.float32)
    row_image = row_products(tile_store, primal.astype(jnp.bfloat16), blocks)
    for iteration in range(ITERS):
        step_primal = step_scale / weight
        step_dual = step_scale * weight
        partial_value = column_products(tile_store, dual_state.astype(jnp.bfloat16))
        gradient = lax.psum(partial_value, ("grp", "dev"))
        primal_next = jnp.clip(primal - step_primal * (cost_vector - gradient), 0.0, upper_bound)
        change = jnp.sum((primal_next - primal) ** 2)
        next_image = row_products(tile_store, primal_next.astype(jnp.bfloat16), blocks)
        dual_state = jnp.maximum(
            dual_state + step_dual * (bounds - (2.0 * next_image - row_image)), 0.0
        )
        violation_part = jnp.sum(jnp.maximum(bounds - next_image, 0.0) ** 2)
        violation = lax.psum(violation_part, ("grp", "dev"))
        weight = jnp.sqrt(weight * jnp.sqrt((violation + 1e-06) / (change + 1e-06)))
        primal = primal_next
        row_image = next_image
    dual_final = lax.all_to_all(
        dual_state[inverse], "dev", split_axis=0, concat_axis=0, tiled=True
    ).reshape(-1)
    return (primal, dual_final, jnp.reshape(weight, (1,)))


MESH_ID = pl.DeviceIdType.MESH
LANES = 128
TILE = 4


def fits(mesh_shape, slots, rows_per, width, blocks, column_blocks):
    n_grp, n_dev = mesh_shape["grp"], mesh_shape["dev"]
    n_chip = n_dev // 2
    if n_dev % 2 or n_chip & (n_chip - 1) or width != n_dev * LANES:
        return False
    if rows_per != LANES or blocks != n_dev or blocks != 8 or slots > 32:
        return False
    if slots % 4 or (n_grp * n_dev * slots) % LANES or column_blocks % LANES:
        return False
    held = slots * rows_per * width * 2 + column_blocks * width * 4 * 5
    return held < 30 * 2**20


def split_kernel(
    n_grp,
    n_dev,
    cols_in,
    counts_in,
    dest_in,
    bounds_in,
    dual_in,
    tiles,
    primal_in,
    cost_in,
    upper_in,
    out_primal,
    out_dual,
    out_weight,
    kv,
    pv,
    cv,
    uv,
    cs,
    us,
    pnow,
    pbf,
    hot,
    hot_back,
    asend,
    abuf,
    bsend,
    bbuf,
    stat,
    fbuf,
    dsend,
    drecv,
    tile_sem,
    local_sem,
    out_sem,
    a_send,
    a_recv,
    b_send,
    b_recv,
    stat_send,
    stat_recv,
    f_send,
    f_recv,
    p_send,
    p_recv,
    dual_send,
    dual_recv,
):
    slots, rows_per, width = tiles.shape
    blocks = bounds_in.shape[0]
    n_cb = pnow.shape[0]
    n_all = n_grp * n_dev
    n_chip = n_dev // 2
    span = 2 * LANES
    packs = slots // TILE
    f32, bf16, i32 = jnp.float32, jnp.bfloat16, jnp.int32
    g = lax.axis_index("grp")
    d = lax.axis_index("dev")
    core = d % 2
    chip = d // 2
    twin = 1 - core
    partner = chip * 2 + twin
    me = g * n_dev + d

    def remote(src, dst, ssem, rsem, tg, td):
        return pltpu.make_async_remote_copy(
            src_ref=src,
            dst_ref=dst,
            send_sem=ssem,
            recv_sem=rsem,
            device_id={"grp": tg, "dev": td},
            device_id_type=MESH_ID,
        )

    def bytes_of(ref, ssem, rsem):
        return remote(ref, ref, ssem, rsem, g, partner)

    others = [(a, b) for a in range(n_grp) for b in range(n_dev) if a or b]

    def other(a, b):
        return (g + a) % n_grp, (d + b) % n_dev

    def chunk(u):
        return pl.ds(pl.multiple_of((chip ^ u) * span, span), span)

    barrier = pltpu.get_barrier_semaphore()
    for a, b in others:
        tg, td = other(a, b)
        pl.semaphore_signal(
            barrier, inc=1, device_id={"grp": tg, "dev": td}, device_id_type=MESH_ID
        )
    order = [u for u in range(n_chip - 1, 0, -1)] + [0]
    part = 4
    for u in order:
        for k in range(0, slots, part):
            pltpu.make_async_copy(
                tiles.at[pl.ds(k, part), :, chunk(u)],
                kv.at[pl.ds(k, part), :, chunk(u)],
                tile_sem.at[u],
            ).start()
    copies = [
        pltpu.make_async_copy(primal_in, pv, local_sem.at[0]),
        pltpu.make_async_copy(cost_in, cv, local_sem.at[1]),
        pltpu.make_async_copy(upper_in, uv, local_sem.at[2]),
    ]
    for copy in copies:
        copy.start()

    cols = [cols_in[k] for k in range(slots)]
    counts = [counts_in[k] for k in range(blocks)]
    dest = [dest_in[k] for k in range(blocks)]
    starts = [counts[0] * 0]
    for b in range(blocks):
        starts.append(starts[-1] + counts[b])
    total = starts[-1]
    live = [jnp.where(s < total, cols[s], -1) for s in range(slots)]
    lane = lax.broadcasted_iota(i32, (1, LANES), 1)
    turn = (me * slots) % LANES
    place = jnp.where(lane < turn, lane - turn + LANES, lane - turn)
    stat_row = jnp.full((1, LANES), -1.0, f32)
    for s in range(slots):
        stat_row = jnp.where(place == s, live[s].astype(f32), stat_row)
    stat[0, me] = stat_row
    rows = 32
    row = lax.broadcasted_iota(i32, (rows, LANES), 0)
    row_owner = jnp.zeros((rows, LANES), i32)
    for b in range(1, blocks):
        row_owner = row_owner + jnp.where(row >= starts[b], 1, 0)
    row_owner = jnp.where(row < total, row_owner, -1)
    own_lane = lax.broadcasted_iota(i32, (blocks, slots), 1)
    own_row = lax.broadcasted_iota(i32, (blocks, slots), 0)
    first = jnp.zeros((blocks, slots), i32)
    last = jnp.zeros((blocks, slots), i32)
    for b in range(blocks):
        first = jnp.where(own_row == b, starts[b], first)
        last = jnp.where(own_row == b, starts[b + 1], last)
    owner_hot = jnp.where((own_lane >= first) & (own_lane < last), 1.0, 0.0).astype(bf16)
    slot_lane = lax.broadcasted_iota(i32, (rows_per, slots), 1)
    bounds = bounds_in[...].astype(f32)
    dual = dual_in[...].astype(f32)

    def pieces(it, dual_now, before):
        spread = jnp.zeros((rows, rows_per), f32)
        for b in range(blocks):
            spread = jnp.where(row_owner == b, dual_now[b : b + 1, :], spread)
        left = [
            jnp.concatenate(
                [jnp.where(row == s, spread, 0.0), jnp.where(row == s + 1, spread, 0.0)],
                axis=1,
            ).astype(bf16)
            for s in range(0, slots, 2)
        ]
        for u in order:
            before(u)
            whole = jnp.zeros((rows, span), f32)
            for s in range(0, slots, 2):
                pair = kv[s : s + 2, :, chunk(u)].reshape(2 * rows_per, span)
                whole = whole + jnp.dot(left[s // 2], pair, preferred_element_type=f32)
            halves = [
                whole[:slots, h * LANES : (h + 1) * LANES].astype(bf16).reshape(packs, TILE, LANES)
                for h in range(2)
            ]
            for h in range(2):
                asend[it, u, h] = halves[h]
            if u == 0:
                abuf[it, pl.ds(me * packs, packs)] = jnp.where(core == 0, halves[0], halves[1])

    def send_pieces(it, u):
        def send(src, tg, td):
            remote(
                src,
                abuf.at[it, pl.ds(me * packs, packs)],
                a_send.at[it],
                a_recv.at[it],
                tg,
                td,
            ).start()

        for a in range(n_grp - 1, 0, -1):
            for h in range(2):
                send(asend.at[it, u, h], (g + a) % n_grp, (chip ^ u) * 2 + h)
        if u:
            for h in range(2):
                send(asend.at[it, u, h], g, (chip ^ u) * 2 + h)
        else:
            send(asend.at[it, 0, twin], g, partner)

    def send_stat(turn_no):
        for a, b in others:
            tg, td = other(a, b)
            remote(
                stat.at[turn_no, me],
                stat.at[turn_no, me],
                stat_send.at[turn_no],
                stat_recv.at[turn_no],
                tg,
                td,
            ).start()

    def stat_bytes(turn_no):
        return bytes_of(
            stat.at[turn_no, pl.ds(0, n_all - 1)], stat_send.at[turn_no], stat_recv.at[turn_no]
        )

    def piece_bytes(it):
        return bytes_of(
            abuf.at[it, pl.ds(0, (n_all - 1) * packs)], a_send.at[it], a_recv.at[it]
        )

    def image_part(acc, picked, lanes):
        for s in range(0, slots, 4):
            block = kv[s : s + 4, :, lanes].reshape(4 * rows_per, span)
            out = lax.dot_general(
                block, picked, (((1,), (1,)), ((), ())), preferred_element_type=f32
            )
            for k in range(4):
                here = out[k * rows_per : (k + 1) * rows_per]
                acc = jnp.where(slot_lane == s + k, acc + here, acc)
        return acc

    def image_of(acc):
        high = acc.astype(bf16)
        rest = acc - high.astype(f32)
        mid = rest.astype(bf16)
        low = (rest - mid.astype(f32)).astype(bf16)
        image = jnp.zeros((blocks, rows_per), f32)
        for term in (high, mid, low):
            image = image + lax.dot_general(
                owner_hot, term, (((1,), (1,)), ((), ())), preferred_element_type=f32
            )
        return image

    def no_image():
        return jnp.zeros((rows_per, slots), f32)

    def first_image():
        copies[0].wait()
        for j in range(n_dev):
            value = pv[pl.ds(j, n_cb, stride=n_dev), :]
            pbf[:, j * LANES : (j + 1) * LANES] = value.astype(bf16)
        pnow[...] = pv[pl.ds(d, n_cb, stride=n_dev), :]
        wide = lax.broadcasted_iota(i32, (rows, n_cb), 0)
        wide_col = jnp.full((rows, n_cb), -1, i32)
        for s in range(slots):
            wide_col = jnp.where(wide == s, live[s], wide_col)
        own_hot = jnp.where(
            wide_col == lax.broadcasted_iota(i32, (rows, n_cb), 1), 1.0, 0.0
        ).astype(bf16)
        picked = jnp.dot(own_hot, pbf[...], preferred_element_type=f32).astype(bf16)[:slots]
        acc = no_image()
        for c in range(n_chip):
            lanes = slice(c * span, (c + 1) * span)
            acc = image_part(acc, picked[:, lanes], lanes)
        return image_of(acc)

    def build_hot():
        stat_bytes(0).wait_recv()
        block_of = lax.broadcasted_iota(i32, (n_cb, LANES), 0).astype(f32)
        for t in range(n_all * slots // LANES):
            line = jnp.full((1, LANES), -1.0, f32)
            for k in range(n_all):
                low, high = k * slots - t * LANES, (k + 1) * slots - t * LANES
                if high > 0 and low < LANES:
                    line = jnp.where((lane >= low) & (lane < high), stat[0, k], line)
            hot[:, t * LANES : (t + 1) * LANES] = jnp.where(block_of == line, 1.0, 0.0).astype(bf16)
        back = n_dev * slots
        back_row = lax.broadcasted_iota(i32, (back, LANES), 0)
        back_lane = lax.broadcasted_iota(i32, (back, LANES), 1)
        back_dev, back_slot = back_row // slots, back_row % slots
        found = jnp.zeros((back, LANES), f32)
        for u in range(n_chip):
            for h in range(2):
                src = g * n_dev + (chip ^ u) * 2 + h
                shift = (src * slots) % LANES
                at = jnp.where(back_lane < shift, back_lane - shift + LANES, back_lane - shift)
                hit = (back_dev == u * 2 + h) & (at == back_slot)
                found = jnp.where(hit, stat[0, src] + 1.0, found)
        wanted = jnp.sum(found, axis=1, keepdims=True) - 1.0
        lane_cb = lax.broadcasted_iota(i32, (back, n_cb), 1).astype(f32)
        hot_back[...] = jnp.where(wanted == lane_cb, 1.0, 0.0).astype(bf16)

    def load_slices():
        copies[1].wait()
        copies[2].wait()
        cs[...] = cv[pl.ds(d, n_cb, stride=n_dev), :]
        us[...] = uv[pl.ds(d, n_cb, stride=n_dev), :]

    weight = jnp.ones((1, 1), f32)
    image = None
    for it in range(ITERS):
        if it == 0:

            def ready(u):
                pltpu.make_async_copy(
                    tiles.at[:, :, chunk(u)], kv.at[:, :, chunk(u)], tile_sem.at[u]
                ).wait()

            pieces(it, dual, ready)
            pl.semaphore_wait(barrier, len(others))
            send_stat(0)
            for u in order:
                send_pieces(it, u)
            image = first_image()
            load_slices()
            build_hot()
        else:
            sent_before = []

            def flow(u):
                if sent_before:
                    send_pieces(it, sent_before[-1])
                sent_before.append(u)

            pieces(it, dual, flow)
            send_pieces(it, sent_before[-1])
            stat_bytes(it).wait_recv()
            violation = jnp.sum(stat[it], axis=0)[:, LANES - 1 :]
            change = jnp.sum(stat[it, 0:n_dev], axis=0)[:, :1]
            weight = jnp.sqrt(weight * jnp.sqrt((violation + 1e-06) / (change + 1e-06)))
        tau = step_scale / weight
        piece_bytes(it).wait_recv()
        grad = jnp.dot(
            hot[...],
            abuf.at[it].reshape(n_all * slots, LANES)[...],
            preferred_element_type=f32,
        )
        old = pnow[...]
        new = jnp.minimum(jnp.maximum(old - tau * (cs[...] - grad), 0.0), us[...])
        back = jnp.dot(hot_back[...], new.astype(bf16), preferred_element_type=f32)
        back = back.astype(bf16).reshape(n_chip, 2, packs, TILE, LANES)
        bsend[it] = back
        bbuf[it, 0, core] = jnp.where(core == 0, back[0, 0], back[0, 1])

        def send_back(src, dst, u, td):
            remote(src, dst, b_send.at[it], b_recv.at[it, u], g, td).start()

        for u in order[:-1]:
            for h in range(2):
                send_back(
                    bsend.at[it, u, h], bbuf.at[it, u, core], u, (chip ^ u) * 2 + h
                )
        send_back(bsend.at[it, 0, twin], bbuf.at[it, 0, core], 0, partner)
        gap = new - old
        moved = jnp.sum(gap * gap, axis=(0, 1), keepdims=True)
        if it < ITERS - 1:
            pnow[...] = new
        else:
            fbuf[0] = new
            for u in order[:-1]:
                remote(
                    fbuf.at[0], fbuf.at[u], f_send.at[0], f_recv.at[u], g, (chip ^ u) * 2 + core
                ).start()
            remote(fbuf.at[0], out_primal.at[d], p_send.at[0], p_recv.at[0], g, partner).start()
            pltpu.make_async_copy(fbuf.at[0], out_primal.at[d], out_sem.at[0]).start()

        acc = no_image()
        for u in range(n_chip):
            one = bbuf.at[it, 0, 0] if u == 0 else bbuf.at[it, u]
            bytes_of(one, b_send.at[it], b_recv.at[it, u]).wait_recv()
            picked = jnp.concatenate(
                [bbuf[it, u, h].reshape(slots, LANES) for h in range(2)], axis=1
            )
            acc = image_part(acc, picked, chunk(u))
        next_image = image_of(acc)
        sigma = step_scale * weight
        dual = jnp.maximum(dual + sigma * (bounds - (2.0 * next_image - image)), 0.0)
        short = jnp.maximum(bounds - next_image, 0.0)
        image = next_image
        missed = jnp.sum(short * short, axis=(0, 1), keepdims=True)
        stat[it + 1, me] = jnp.where(lane < LANES // 2, moved, missed)
        send_stat(it + 1)

    for e in range(n_dev):
        line = jnp.zeros((1, rows_per), f32)
        for k in range(blocks):
            line = jnp.where(dest[k] == e, dual[k : k + 1, :], line)
        dsend[e] = line
    for k in range(1, n_dev):
        td = (d + k) % n_dev
        remote(dsend.at[td], drecv.at[d], dual_send.at[0], dual_recv.at[0], g, td).start()
    drecv[d] = dsend[d]
    for u in range(1, n_chip):
        bytes_of(fbuf.at[u], f_send.at[0], f_recv.at[u]).wait_recv()
        src = (chip ^ u) * 2 + core
        remote(fbuf.at[u], out_primal.at[src], p_send.at[0], p_recv.at[0], g, partner).start()
        pltpu.make_async_copy(fbuf.at[u], out_primal.at[src], out_sem.at[0]).start()
    bytes_of(drecv.at[pl.ds(0, n_dev - 1)], dual_send.at[0], dual_recv.at[0]).wait_recv()
    out_dual[...] = drecv[...]
    stat_bytes(ITERS).wait_recv()
    violation = jnp.sum(stat[ITERS], axis=0)[:, LANES - 1 :]
    change = jnp.sum(stat[ITERS, 0:n_dev], axis=0)[:, :1]
    weight = jnp.sqrt(weight * jnp.sqrt((violation + 1e-06) / (change + 1e-06)))
    out_weight[...] = jnp.broadcast_to(weight, (1, LANES))
    for it in range(ITERS):
        piece_bytes(it).wait_send()
        bytes_of(
            bbuf.at[it, pl.ds(0, n_chip - 1)], b_send.at[it], b_recv.at[it, 0]
        ).wait_send()
        bytes_of(bbuf.at[it, 0, 0], b_send.at[it], b_recv.at[it, 0]).wait_send()
    for turn_no in range(ITERS + 1):
        stat_bytes(turn_no).wait_send()
    bytes_of(drecv.at[pl.ds(0, n_dev - 1)], dual_send.at[0], dual_recv.at[0]).wait_send()
    bytes_of(fbuf.at[pl.ds(0, n_chip - 1)], f_send.at[0], f_recv.at[0]).wait_send()
    bytes_of(fbuf, p_send.at[0], p_recv.at[0]).wait_send()
    bytes_of(fbuf, p_send.at[0], p_recv.at[0]).wait_recv()
    pltpu.make_async_copy(fbuf, out_primal.at[pl.ds(0, n_chip)], out_sem.at[0]).wait()


def split_device(mesh_shape, *args):
    tiles, cols, counts, dest, row_bounds, dual_start, primal, cost, upper = args
    slots, rows_per, width = tiles.shape
    blocks = counts.shape[0]
    n_cb = primal.shape[0] // width
    if not fits(mesh_shape, slots, rows_per, width, blocks, n_cb):
        return per_device(*args)
    n_grp, n_dev = mesh_shape["grp"], mesh_shape["dev"]
    n_all, n_chip = n_grp * n_dev, n_dev // 2
    packs = slots // TILE
    flat = (primal.shape[0] // LANES, LANES)
    f32, bf16 = jnp.float32, jnp.bfloat16
    vmem = pl.BlockSpec(memory_space=pltpu.VMEM)
    smem = pl.BlockSpec(memory_space=pltpu.SMEM)
    far = pl.BlockSpec(memory_space=pltpu.HBM)
    dma = pltpu.SemaphoreType.DMA
    out_primal, out_dual, out_weight = pl.pallas_call(
        functools.partial(split_kernel, n_grp, n_dev),
        name="pdhg_split",
        out_shape=(
            jax.ShapeDtypeStruct((n_dev, n_cb, LANES), f32),
            jax.ShapeDtypeStruct((n_dev, 1, rows_per), f32),
            jax.ShapeDtypeStruct((1, LANES), f32),
        ),
        in_specs=[smem, smem, smem, vmem, vmem, far, far, far, far],
        out_specs=(far, vmem, vmem),
        scratch_shapes=[
            pltpu.VMEM((slots, rows_per, width), bf16),
            pltpu.VMEM(flat, f32),
            pltpu.VMEM(flat, f32),
            pltpu.VMEM(flat, f32),
            pltpu.VMEM((n_cb, LANES), f32),
            pltpu.VMEM((n_cb, LANES), f32),
            pltpu.VMEM((n_cb, LANES), f32),
            pltpu.VMEM((n_cb, width), bf16),
            pltpu.VMEM((n_cb, n_all * slots), bf16),
            pltpu.VMEM((n_dev * slots, n_cb), bf16),
            pltpu.VMEM((ITERS, n_chip, 2, packs, TILE, LANES), bf16),
            pltpu.VMEM((ITERS, n_all * packs, TILE, LANES), bf16),
            pltpu.VMEM((ITERS, n_chip, 2, packs, TILE, LANES), bf16),
            pltpu.VMEM((ITERS, n_chip, 2, packs, TILE, LANES), bf16),
            pltpu.VMEM((ITERS + 1, n_all, 1, LANES), f32),
            pltpu.VMEM((n_chip, n_cb, LANES), f32),
            pltpu.VMEM((n_dev, 1, rows_per), f32),
            pltpu.VMEM((n_dev, 1, rows_per), f32),
            dma((n_chip,)),
            dma((3,)),
            dma((1,)),
            dma((ITERS,)),
            dma((ITERS,)),
            dma((ITERS,)),
            dma((ITERS, n_chip)),
            dma((ITERS + 1,)),
            dma((ITERS + 1,)),
            dma((1,)),
            dma((n_chip,)),
            dma((1,)),
            dma((1,)),
            dma((1,)),
            dma((1,)),
        ],
        compiler_params=pltpu.CompilerParams(
            collective_id=0, has_side_effects=True, vmem_limit_bytes=50 * 10**6
        ),
    )(
        cols,
        counts,
        dest,
        row_bounds.reshape(blocks, rows_per),
        dual_start.reshape(blocks, rows_per),
        tiles,
        primal.reshape(flat),
        cost.reshape(flat),
        upper.reshape(flat),
    )
    primal_final = out_primal.transpose(1, 0, 2).reshape(-1)
    return primal_final, out_dual.reshape(-1), out_weight[0, :1]


def solution(mesh):
    in_specs = (
        P(("grp", "dev"), None, None),
        P(("grp", "dev")),
        P(("grp", "dev")),
        P(("grp", "dev")),
        P(("grp", "dev")),
        P(("grp", "dev")),
        P(),
        P(),
        P(),
    )
    out_specs = (P(), P(("grp", "dev")), P())
    return jax.shard_map(
        functools.partial(split_device, dict(mesh.shape)),
        mesh=mesh,
        in_specs=in_specs,
        out_specs=out_specs,
        check_vma=False,
    )
```

```python
import functools

import jax
import jax.numpy as jnp
from jax import lax
from jax.experimental import pallas as pl
from jax.experimental.pallas import tpu as pltpu
from jax.sharding import PartitionSpec as P

NCB = 256
ITERS = 3


step_scale = 0.3


def row_products(tile_store, vector_bf, blocks):
    tile_set, tile_cols, owners, live_flags = tile_store
    vector_table = vector_bf.reshape(-1, tile_set.shape[2])
    column_hot = (
        tile_cols[:, None] == jnp.arange(vector_table.shape[0], dtype=jnp.int32)[None, :]
    ).astype(jnp.bfloat16)
    picked = jnp.dot(column_hot, vector_table, preferred_element_type=jnp.float32).astype(
        jnp.bfloat16
    )
    product = jnp.einsum("src,sc->sr", tile_set, picked, preferred_element_type=jnp.float32)
    product = jnp.where(live_flags[:, None], product, 0.0)
    owner_hot = (jnp.arange(blocks, dtype=jnp.int32)[:, None] == owners[None, :]).astype(
        jnp.float32
    )
    return jnp.dot(owner_hot, product, precision=lax.Precision.HIGHEST)


def column_products(tile_store, rows_bf):
    tile_set, tile_cols, owners, live_flags = tile_store
    blocks = rows_bf.shape[0]
    owner_hot = (owners[:, None] == jnp.arange(blocks, dtype=jnp.int32)[None, :]).astype(
        jnp.bfloat16
    )
    picked_rows = jnp.dot(owner_hot, rows_bf, preferred_element_type=jnp.float32).astype(
        jnp.bfloat16
    )
    product = jnp.einsum("src,sr->sc", tile_set, picked_rows, preferred_element_type=jnp.float32)
    product = jnp.where(live_flags[:, None], product, 0.0)
    column_hot = (jnp.arange(NCB, dtype=jnp.int32)[:, None] == tile_cols[None, :]).astype(
        jnp.float32
    )
    return jnp.dot(column_hot, product, precision=lax.Precision.HIGHEST).reshape(-1)


def per_device(
    matrix_tiles,
    tile_column,
    block_counts,
    destination,
    row_bounds,
    dual_start,
    primal_start,
    cost_vector,
    upper_bound,
):
    blocks = block_counts.shape[0]
    rows_per = matrix_tiles.shape[1]
    slot_count = matrix_tiles.shape[0]
    starts = jnp.cumsum(block_counts) - block_counts
    slot_ids = jnp.arange(slot_count, dtype=jnp.int32)
    owners = jnp.sum((starts[None, 1:] <= slot_ids[:, None]).astype(jnp.int32), axis=1)
    bounds_here = row_bounds.reshape(blocks, rows_per)
    dual_here = dual_start.reshape(blocks, rows_per)
    peer_ids = jnp.arange(blocks, dtype=jnp.int32)
    inverse = jnp.sum(
        jnp.where(destination[None, :] == peer_ids[:, None], peer_ids[None, :], 0), axis=1
    )
    tile_store = (matrix_tiles, tile_column, owners, slot_ids < jnp.sum(block_counts))
    bounds = bounds_here.astype(jnp.float32)
    dual_state = dual_here.astype(jnp.float32)
    primal = primal_start
    weight = jnp.ones((), jnp.float32)
    row_image = row_products(tile_store, primal.astype(jnp.bfloat16), blocks)
    for iteration in range(ITERS):
        step_primal = step_scale / weight
        step_dual = step_scale * weight
        partial_value = column_products(tile_store, dual_state.astype(jnp.bfloat16))
        gradient = lax.psum(partial_value, ("grp", "dev"))
        primal_next = jnp.clip(primal - step_primal * (cost_vector - gradient), 0.0, upper_bound)
        change = jnp.sum((primal_next - primal) ** 2)
        next_image = row_products(tile_store, primal_next.astype(jnp.bfloat16), blocks)
        dual_state = jnp.maximum(
            dual_state + step_dual * (bounds - (2.0 * next_image - row_image)), 0.0
        )
        violation_part = jnp.sum(jnp.maximum(bounds - next_image, 0.0) ** 2)
        violation = lax.psum(violation_part, ("grp", "dev"))
        weight = jnp.sqrt(weight * jnp.sqrt((violation + 1e-06) / (change + 1e-06)))
        primal = primal_next
        row_image = next_image
    dual_final = lax.all_to_all(
        dual_state[inverse], "dev", split_axis=0, concat_axis=0, tiled=True
    ).reshape(-1)
    return (primal, dual_final, jnp.reshape(weight, (1,)))


MESH_ID = pl.DeviceIdType.MESH
LANES = 128
TILE = 4


def fits(mesh_shape, slots, rows_per, width, blocks, column_blocks):
    n_grp, n_dev = mesh_shape["grp"], mesh_shape["dev"]
    n_chip = n_dev // 2
    if n_dev % 2 or n_chip & (n_chip - 1) or width != n_dev * LANES:
        return False
    if rows_per != LANES or blocks != n_dev or blocks != 8 or slots > 32:
        return False
    if slots % 4 or (n_grp * n_dev * slots) % LANES or column_blocks % LANES:
        return False
    held = slots * rows_per * width * 2 + column_blocks * width * 4 * 5
    return held < 30 * 2**20


def split_kernel(
    n_grp,
    n_dev,
    cols_in,
    counts_in,
    dest_in,
    bounds_in,
    dual_in,
    tiles,
    primal_in,
    cost_in,
    upper_in,
    out_primal,
    out_dual,
    out_weight,
    kv,
    pv,
    cv,
    uv,
    cs,
    us,
    pnow,
    pbf,
    hot,
    hot_back,
    asend,
    abuf,
    bsend,
    bbuf,
    stat,
    fbuf,
    dsend,
    drecv,
    cols_at,
    counts_at,
    dest_at,
    bounds_at,
    dual_at,
    tile_sem,
    local_sem,
    small_sem,
    out_sem,
    a_send,
    a_recv,
    b_send,
    b_recv,
    stat_send,
    stat_recv,
    f_send,
    f_recv,
    p_send,
    p_recv,
    dual_send,
    dual_recv,
):
    slots, rows_per, width = tiles.shape
    blocks = bounds_in.shape[0]
    n_cb = pnow.shape[0]
    n_all = n_grp * n_dev
    n_chip = n_dev // 2
    span = 2 * LANES
    packs = slots // TILE
    f32, bf16, i32 = jnp.float32, jnp.bfloat16, jnp.int32
    g = lax.axis_index("grp")
    d = lax.axis_index("dev")
    core = d % 2
    chip = d // 2
    twin = 1 - core
    partner = chip * 2 + twin
    me = g * n_dev + d

    def remote(src, dst, ssem, rsem, tg, td):
        return pltpu.make_async_remote_copy(
            src_ref=src,
            dst_ref=dst,
            send_sem=ssem,
            recv_sem=rsem,
            device_id={"grp": tg, "dev": td},
            device_id_type=MESH_ID,
        )

    def bytes_of(ref, ssem, rsem):
        return remote(ref, ref, ssem, rsem, g, partner)

    others = [(a, b) for a in range(n_grp) for b in range(n_dev) if a or b]

    def other(a, b):
        return (g + a) % n_grp, (d + b) % n_dev

    def chunk(u):
        return pl.ds(pl.multiple_of((chip ^ u) * span, span), span)

    barrier = pltpu.get_barrier_semaphore()
    for a, b in others:
        tg, td = other(a, b)
        pl.semaphore_signal(
            barrier, inc=1, device_id={"grp": tg, "dev": td}, device_id_type=MESH_ID
        )
    small = [
        pltpu.make_async_copy(src, dst, small_sem.at[k])
        for k, (src, dst) in enumerate(
            (
                (cols_in, cols_at),
                (counts_in, counts_at),
                (dest_in, dest_at),
                (bounds_in, bounds_at),
                (dual_in, dual_at),
            )
        )
    ]
    for copy in small:
        copy.start()
    order = [u for u in range(n_chip - 1, 0, -1)] + [0]
    part = 4
    for u in order:
        for k in range(0, slots, part):
            pltpu.make_async_copy(
                tiles.at[pl.ds(k, part), :, chunk(u)],
                kv.at[pl.ds(k, part), :, chunk(u)],
                tile_sem.at[u],
            ).start()
    copies = [
        pltpu.make_async_copy(primal_in, pv, local_sem.at[0]),
        pltpu.make_async_copy(cost_in, cv, local_sem.at[1]),
        pltpu.make_async_copy(upper_in, uv, local_sem.at[2]),
    ]
    for copy in copies:
        copy.start()

    for copy in small:
        copy.wait()
    cols = [cols_at[k] for k in range(slots)]
    counts = [counts_at[k] for k in range(blocks)]
    dest = [dest_at[k] for k in range(blocks)]
    starts = [counts[0] * 0]
    for b in range(blocks):
        starts.append(starts[-1] + counts[b])
    total = starts[-1]
    live = [jnp.where(s < total, cols[s], -1) for s in range(slots)]
    lane = lax.broadcasted_iota(i32, (1, LANES), 1)
    turn = (me * slots) % LANES
    place = jnp.where(lane < turn, lane - turn + LANES, lane - turn)
    stat_row = jnp.full((1, LANES), -1.0, f32)
    for s in range(slots):
        stat_row = jnp.where(place == s, live[s].astype(f32), stat_row)
    stat[0, me] = stat_row
    rows = 32
    row = lax.broadcasted_iota(i32, (rows, LANES), 0)
    row_owner = jnp.zeros((rows, LANES), i32)
    for b in range(1, blocks):
        row_owner = row_owner + jnp.where(row >= starts[b], 1, 0)
    row_owner = jnp.where(row < total, row_owner, -1)
    own_lane = lax.broadcasted_iota(i32, (blocks, slots), 1)
    own_row = lax.broadcasted_iota(i32, (blocks, slots), 0)
    first = jnp.zeros((blocks, slots), i32)
    last = jnp.zeros((blocks, slots), i32)
    for b in range(blocks):
        first = jnp.where(own_row == b, starts[b], first)
        last = jnp.where(own_row == b, starts[b + 1], last)
    owner_hot = jnp.where((own_lane >= first) & (own_lane < last), 1.0, 0.0).astype(bf16)
    slot_lane = lax.broadcasted_iota(i32, (rows_per, slots), 1)
    bounds = bounds_at[...].astype(f32)
    dual = dual_at[...].astype(f32)

    def pieces(it, dual_now, before):
        spread = jnp.zeros((rows, rows_per), f32)
        for b in range(blocks):
            spread = jnp.where(row_owner == b, dual_now[b : b + 1, :], spread)
        left = [
            jnp.concatenate(
                [jnp.where(row == s, spread, 0.0), jnp.where(row == s + 1, spread, 0.0)],
                axis=1,
            ).astype(bf16)
            for s in range(0, slots, 2)
        ]
        for u in order:
            before(u)
            whole = jnp.zeros((rows, span), f32)
            for s in range(0, slots, 2):
                pair = kv[s : s + 2, :, chunk(u)].reshape(2 * rows_per, span)
                whole = whole + jnp.dot(left[s // 2], pair, preferred_element_type=f32)
            halves = [
                whole[:slots, h * LANES : (h + 1) * LANES].astype(bf16).reshape(packs, TILE, LANES)
                for h in range(2)
            ]
            for h in range(2):
                asend[it, u, h] = halves[h]
            if u == 0:
                abuf[it, pl.ds(me * packs, packs)] = jnp.where(core == 0, halves[0], halves[1])

    def send_pieces(it, u):
        def send(src, tg, td):
            remote(
                src,
                abuf.at[it, pl.ds(me * packs, packs)],
                a_send.at[it],
                a_recv.at[it],
                tg,
                td,
            ).start()

        for a in range(n_grp - 1, 0, -1):
            for h in range(2):
                send(asend.at[it, u, h], (g + a) % n_grp, (chip ^ u) * 2 + h)
        if u:
            for h in range(2):
                send(asend.at[it, u, h], g, (chip ^ u) * 2 + h)
        else:
            send(asend.at[it, 0, twin], g, partner)

    def send_stat(turn_no):
        for a, b in others:
            tg, td = other(a, b)
            remote(
                stat.at[turn_no, me],
                stat.at[turn_no, me],
                stat_send.at[turn_no],
                stat_recv.at[turn_no],
                tg,
                td,
            ).start()

    def stat_bytes(turn_no):
        return bytes_of(
            stat.at[turn_no, pl.ds(0, n_all - 1)], stat_send.at[turn_no], stat_recv.at[turn_no]
        )

    def piece_bytes(it):
        return bytes_of(
            abuf.at[it, pl.ds(0, (n_all - 1) * packs)], a_send.at[it], a_recv.at[it]
        )

    def image_part(acc, picked, lanes):
        for s in range(0, slots, 4):
            block = kv[s : s + 4, :, lanes].reshape(4 * rows_per, span)
            out = lax.dot_general(
                block, picked, (((1,), (1,)), ((), ())), preferred_element_type=f32
            )
            for k in range(4):
                here = out[k * rows_per : (k + 1) * rows_per]
                acc = jnp.where(slot_lane == s + k, acc + here, acc)
        return acc

    def image_of(acc):
        high = acc.astype(bf16)
        rest = acc - high.astype(f32)
        mid = rest.astype(bf16)
        low = (rest - mid.astype(f32)).astype(bf16)
        image = jnp.zeros((blocks, rows_per), f32)
        for term in (high, mid, low):
            image = image + lax.dot_general(
                owner_hot, term, (((1,), (1,)), ((), ())), preferred_element_type=f32
            )
        return image

    def no_image():
        return jnp.zeros((rows_per, slots), f32)

    def first_image():
        copies[0].wait()
        for j in range(n_dev):
            value = pv[pl.ds(j, n_cb, stride=n_dev), :]
            pbf[:, j * LANES : (j + 1) * LANES] = value.astype(bf16)
        pnow[...] = pv[pl.ds(d, n_cb, stride=n_dev), :]
        wide = lax.broadcasted_iota(i32, (rows, n_cb), 0)
        wide_col = jnp.full((rows, n_cb), -1, i32)
        for s in range(slots):
            wide_col = jnp.where(wide == s, live[s], wide_col)
        own_hot = jnp.where(
            wide_col == lax.broadcasted_iota(i32, (rows, n_cb), 1), 1.0, 0.0
        ).astype(bf16)
        picked = jnp.dot(own_hot, pbf[...], preferred_element_type=f32).astype(bf16)[:slots]
        acc = no_image()
        for c in range(n_chip):
            lanes = slice(c * span, (c + 1) * span)
            acc = image_part(acc, picked[:, lanes], lanes)
        return image_of(acc)

    def build_hot():
        stat_bytes(0).wait_recv()
        block_of = lax.broadcasted_iota(i32, (n_cb, LANES), 0).astype(f32)
        for t in range(n_all * slots // LANES):
            line = jnp.full((1, LANES), -1.0, f32)
            for k in range(n_all):
                low, high = k * slots - t * LANES, (k + 1) * slots - t * LANES
                if high > 0 and low < LANES:
                    line = jnp.where((lane >= low) & (lane < high), stat[0, k], line)
            hot[:, t * LANES : (t + 1) * LANES] = jnp.where(block_of == line, 1.0, 0.0).astype(bf16)
        back = n_dev * slots
        back_row = lax.broadcasted_iota(i32, (back, LANES), 0)
        back_lane = lax.broadcasted_iota(i32, (back, LANES), 1)
        back_dev, back_slot = back_row // slots, back_row % slots
        found = jnp.zeros((back, LANES), f32)
        for u in range(n_chip):
            for h in range(2):
                src = g * n_dev + (chip ^ u) * 2 + h
                shift = (src * slots) % LANES
                at = jnp.where(back_lane < shift, back_lane - shift + LANES, back_lane - shift)
                hit = (back_dev == u * 2 + h) & (at == back_slot)
                found = jnp.where(hit, stat[0, src] + 1.0, found)
        wanted = jnp.sum(found, axis=1, keepdims=True) - 1.0
        lane_cb = lax.broadcasted_iota(i32, (back, n_cb), 1).astype(f32)
        hot_back[...] = jnp.where(wanted == lane_cb, 1.0, 0.0).astype(bf16)

    def load_slices():
        copies[1].wait()
        copies[2].wait()
        cs[...] = cv[pl.ds(d, n_cb, stride=n_dev), :]
        us[...] = uv[pl.ds(d, n_cb, stride=n_dev), :]

    weight = jnp.ones((1, 1), f32)
    image = None
    for it in range(ITERS):
        if it == 0:

            def ready(u):
                pltpu.make_async_copy(
                    tiles.at[:, :, chunk(u)], kv.at[:, :, chunk(u)], tile_sem.at[u]
                ).wait()

            pieces(it, dual, ready)
            pl.semaphore_wait(barrier, len(others))
            send_stat(0)
            for u in order:
                send_pieces(it, u)
            image = first_image()
            load_slices()
            build_hot()
        else:
            sent_before = []

            def flow(u):
                if sent_before:
                    send_pieces(it, sent_before[-1])
                sent_before.append(u)

            pieces(it, dual, flow)
            send_pieces(it, sent_before[-1])
            stat_bytes(it).wait_recv()
            violation = jnp.sum(stat[it], axis=0)[:, LANES - 1 :]
            change = jnp.sum(stat[it, 0:n_dev], axis=0)[:, :1]
            weight = jnp.sqrt(weight * jnp.sqrt((violation + 1e-06) / (change + 1e-06)))
        tau = step_scale / weight
        piece_bytes(it).wait_recv()
        grad = jnp.dot(
            hot[...],
            abuf.at[it].reshape(n_all * slots, LANES)[...],
            preferred_element_type=f32,
        )
        old = pnow[...]
        new = jnp.minimum(jnp.maximum(old - tau * (cs[...] - grad), 0.0), us[...])
        back = jnp.dot(hot_back[...], new.astype(bf16), preferred_element_type=f32)
        back = back.astype(bf16).reshape(n_chip, 2, packs, TILE, LANES)
        bsend[it] = back
        bbuf[it, 0, core] = jnp.where(core == 0, back[0, 0], back[0, 1])

        def send_back(src, dst, u, td):
            remote(src, dst, b_send.at[it], b_recv.at[it, u], g, td).start()

        for u in order[:-1]:
            for h in range(2):
                send_back(
                    bsend.at[it, u, h], bbuf.at[it, u, core], u, (chip ^ u) * 2 + h
                )
        send_back(bsend.at[it, 0, twin], bbuf.at[it, 0, core], 0, partner)
        gap = new - old
        moved = jnp.sum(gap * gap, axis=(0, 1), keepdims=True)
        if it < ITERS - 1:
            pnow[...] = new
        else:
            fbuf[0] = new
            for u in order[:-1]:
                remote(
                    fbuf.at[0], fbuf.at[u], f_send.at[0], f_recv.at[u], g, (chip ^ u) * 2 + core
                ).start()
            remote(fbuf.at[0], out_primal.at[d], p_send.at[0], p_recv.at[0], g, partner).start()
            pltpu.make_async_copy(fbuf.at[0], out_primal.at[d], out_sem.at[0]).start()

        acc = no_image()
        for u in range(n_chip):
            one = bbuf.at[it, 0, 0] if u == 0 else bbuf.at[it, u]
            bytes_of(one, b_send.at[it], b_recv.at[it, u]).wait_recv()
            picked = jnp.concatenate(
                [bbuf[it, u, h].reshape(slots, LANES) for h in range(2)], axis=1
            )
            acc = image_part(acc, picked, chunk(u))
        next_image = image_of(acc)
        sigma = step_scale * weight
        dual = jnp.maximum(dual + sigma * (bounds - (2.0 * next_image - image)), 0.0)
        short = jnp.maximum(bounds - next_image, 0.0)
        image = next_image
        missed = jnp.sum(short * short, axis=(0, 1), keepdims=True)
        stat[it + 1, me] = jnp.where(lane < LANES // 2, moved, missed)
        send_stat(it + 1)

    for e in range(n_dev):
        line = jnp.zeros((1, rows_per), f32)
        for k in range(blocks):
            line = jnp.where(dest[k] == e, dual[k : k + 1, :], line)
        dsend[e] = line
    for k in range(1, n_dev):
        td = (d + k) % n_dev
        remote(dsend.at[td], drecv.at[d], dual_send.at[0], dual_recv.at[0], g, td).start()
    drecv[d] = dsend[d]
    for u in range(1, n_chip):
        bytes_of(fbuf.at[u], f_send.at[0], f_recv.at[u]).wait_recv()
        src = (chip ^ u) * 2 + core
        remote(fbuf.at[u], out_primal.at[src], p_send.at[0], p_recv.at[0], g, partner).start()
        pltpu.make_async_copy(fbuf.at[u], out_primal.at[src], out_sem.at[0]).start()
    bytes_of(drecv.at[pl.ds(0, n_dev - 1)], dual_send.at[0], dual_recv.at[0]).wait_recv()
    out_dual[...] = drecv[...]
    stat_bytes(ITERS).wait_recv()
    violation = jnp.sum(stat[ITERS], axis=0)[:, LANES - 1 :]
    change = jnp.sum(stat[ITERS, 0:n_dev], axis=0)[:, :1]
    weight = jnp.sqrt(weight * jnp.sqrt((violation + 1e-06) / (change + 1e-06)))
    out_weight[...] = jnp.broadcast_to(weight, (1, LANES))
    for it in range(ITERS):
        piece_bytes(it).wait_send()
        bytes_of(
            bbuf.at[it, pl.ds(0, n_chip - 1)], b_send.at[it], b_recv.at[it, 0]
        ).wait_send()
        bytes_of(bbuf.at[it, 0, 0], b_send.at[it], b_recv.at[it, 0]).wait_send()
    for turn_no in range(ITERS + 1):
        stat_bytes(turn_no).wait_send()
    bytes_of(drecv.at[pl.ds(0, n_dev - 1)], dual_send.at[0], dual_recv.at[0]).wait_send()
    bytes_of(fbuf.at[pl.ds(0, n_chip - 1)], f_send.at[0], f_recv.at[0]).wait_send()
    bytes_of(fbuf, p_send.at[0], p_recv.at[0]).wait_send()
    bytes_of(fbuf, p_send.at[0], p_recv.at[0]).wait_recv()
    pltpu.make_async_copy(fbuf, out_primal.at[pl.ds(0, n_chip)], out_sem.at[0]).wait()


def split_device(mesh_shape, *args):
    tiles, cols, counts, dest, row_bounds, dual_start, primal, cost, upper = args
    slots, rows_per, width = tiles.shape
    blocks = counts.shape[0]
    n_cb = primal.shape[0] // width
    if not fits(mesh_shape, slots, rows_per, width, blocks, n_cb):
        return per_device(*args)
    n_grp, n_dev = mesh_shape["grp"], mesh_shape["dev"]
    n_all, n_chip = n_grp * n_dev, n_dev // 2
    packs = slots // TILE
    flat = (primal.shape[0] // LANES, LANES)
    f32, bf16 = jnp.float32, jnp.bfloat16
    vmem = pl.BlockSpec(memory_space=pltpu.VMEM)
    far = pl.BlockSpec(memory_space=pltpu.HBM)
    dma = pltpu.SemaphoreType.DMA
    out_primal, out_dual, out_weight = pl.pallas_call(
        functools.partial(split_kernel, n_grp, n_dev),
        name="pdhg_split",
        out_shape=(
            jax.ShapeDtypeStruct((n_dev, n_cb, LANES), f32),
            jax.ShapeDtypeStruct((n_dev, 1, rows_per), f32),
            jax.ShapeDtypeStruct((1, LANES), f32),
        ),
        in_specs=[far] * 9,
        out_specs=(far, vmem, vmem),
        scratch_shapes=[
            pltpu.VMEM((slots, rows_per, width), bf16),
            pltpu.VMEM(flat, f32),
            pltpu.VMEM(flat, f32),
            pltpu.VMEM(flat, f32),
            pltpu.VMEM((n_cb, LANES), f32),
            pltpu.VMEM((n_cb, LANES), f32),
            pltpu.VMEM((n_cb, LANES), f32),
            pltpu.VMEM((n_cb, width), bf16),
            pltpu.VMEM((n_cb, n_all * slots), bf16),
            pltpu.VMEM((n_dev * slots, n_cb), bf16),
            pltpu.VMEM((ITERS, n_chip, 2, packs, TILE, LANES), bf16),
            pltpu.VMEM((ITERS, n_all * packs, TILE, LANES), bf16),
            pltpu.VMEM((ITERS, n_chip, 2, packs, TILE, LANES), bf16),
            pltpu.VMEM((ITERS, n_chip, 2, packs, TILE, LANES), bf16),
            pltpu.VMEM((ITERS + 1, n_all, 1, LANES), f32),
            pltpu.VMEM((n_chip, n_cb, LANES), f32),
            pltpu.VMEM((n_dev, 1, rows_per), f32),
            pltpu.VMEM((n_dev, 1, rows_per), f32),
            pltpu.SMEM((slots,), jnp.int32),
            pltpu.SMEM((blocks,), jnp.int32),
            pltpu.SMEM((blocks,), jnp.int32),
            pltpu.VMEM((blocks, rows_per), bf16),
            pltpu.VMEM((blocks, rows_per), bf16),
            dma((n_chip,)),
            dma((3,)),
            dma((5,)),
            dma((1,)),
            dma((ITERS,)),
            dma((ITERS,)),
            dma((ITERS,)),
            dma((ITERS, n_chip)),
            dma((ITERS + 1,)),
            dma((ITERS + 1,)),
            dma((1,)),
            dma((n_chip,)),
            dma((1,)),
            dma((1,)),
            dma((1,)),
            dma((1,)),
        ],
        compiler_params=pltpu.CompilerParams(
            collective_id=0, has_side_effects=True, vmem_limit_bytes=50 * 10**6
        ),
    )(
        cols,
        counts,
        dest,
        row_bounds.reshape(blocks, rows_per),
        dual_start.reshape(blocks, rows_per),
        tiles,
        primal.reshape(flat),
        cost.reshape(flat),
        upper.reshape(flat),
    )
    primal_final = out_primal.transpose(1, 0, 2).reshape(-1)
    return primal_final, out_dual.reshape(-1), out_weight[0, :1]


def solution(mesh):
    in_specs = (
        P(("grp", "dev"), None, None),
        P(("grp", "dev")),
        P(("grp", "dev")),
        P(("grp", "dev")),
        P(("grp", "dev")),
        P(("grp", "dev")),
        P(),
        P(),
        P(),
    )
    out_specs = (P(), P(("grp", "dev")), P())
    return jax.shard_map(
        functools.partial(split_device, dict(mesh.shape)),
        mesh=mesh,
        in_specs=in_specs,
        out_specs=out_specs,
        check_vma=False,
    )
```

```python
import functools

import jax
import jax.numpy as jnp
from jax import lax
from jax.experimental import pallas as pl
from jax.experimental.pallas import tpu as pltpu
from jax.sharding import PartitionSpec as P

NCB = 256
ITERS = 3


step_scale = 0.3


def row_products(tile_store, vector_bf, blocks):
    tile_set, tile_cols, owners, live_flags = tile_store
    vector_table = vector_bf.reshape(-1, tile_set.shape[2])
    column_hot = (
        tile_cols[:, None] == jnp.arange(vector_table.shape[0], dtype=jnp.int32)[None, :]
    ).astype(jnp.bfloat16)
    picked = jnp.dot(column_hot, vector_table, preferred_element_type=jnp.float32).astype(
        jnp.bfloat16
    )
    product = jnp.einsum("src,sc->sr", tile_set, picked, preferred_element_type=jnp.float32)
    product = jnp.where(live_flags[:, None], product, 0.0)
    owner_hot = (jnp.arange(blocks, dtype=jnp.int32)[:, None] == owners[None, :]).astype(
        jnp.float32
    )
    return jnp.dot(owner_hot, product, precision=lax.Precision.HIGHEST)


def column_products(tile_store, rows_bf):
    tile_set, tile_cols, owners, live_flags = tile_store
    blocks = rows_bf.shape[0]
    owner_hot = (owners[:, None] == jnp.arange(blocks, dtype=jnp.int32)[None, :]).astype(
        jnp.bfloat16
    )
    picked_rows = jnp.dot(owner_hot, rows_bf, preferred_element_type=jnp.float32).astype(
        jnp.bfloat16
    )
    product = jnp.einsum("src,sr->sc", tile_set, picked_rows, preferred_element_type=jnp.float32)
    product = jnp.where(live_flags[:, None], product, 0.0)
    column_hot = (jnp.arange(NCB, dtype=jnp.int32)[:, None] == tile_cols[None, :]).astype(
        jnp.float32
    )
    return jnp.dot(column_hot, product, precision=lax.Precision.HIGHEST).reshape(-1)


def per_device(
    matrix_tiles,
    tile_column,
    block_counts,
    destination,
    row_bounds,
    dual_start,
    primal_start,
    cost_vector,
    upper_bound,
):
    blocks = block_counts.shape[0]
    rows_per = matrix_tiles.shape[1]
    slot_count = matrix_tiles.shape[0]
    starts = jnp.cumsum(block_counts) - block_counts
    slot_ids = jnp.arange(slot_count, dtype=jnp.int32)
    owners = jnp.sum((starts[None, 1:] <= slot_ids[:, None]).astype(jnp.int32), axis=1)
    bounds_here = row_bounds.reshape(blocks, rows_per)
    dual_here = dual_start.reshape(blocks, rows_per)
    peer_ids = jnp.arange(blocks, dtype=jnp.int32)
    inverse = jnp.sum(
        jnp.where(destination[None, :] == peer_ids[:, None], peer_ids[None, :], 0), axis=1
    )
    tile_store = (matrix_tiles, tile_column, owners, slot_ids < jnp.sum(block_counts))
    bounds = bounds_here.astype(jnp.float32)
    dual_state = dual_here.astype(jnp.float32)
    primal = primal_start
    weight = jnp.ones((), jnp.float32)
    row_image = row_products(tile_store, primal.astype(jnp.bfloat16), blocks)
    for iteration in range(ITERS):
        step_primal = step_scale / weight
        step_dual = step_scale * weight
        partial_value = column_products(tile_store, dual_state.astype(jnp.bfloat16))
        gradient = lax.psum(partial_value, ("grp", "dev"))
        primal_next = jnp.clip(primal - step_primal * (cost_vector - gradient), 0.0, upper_bound)
        change = jnp.sum((primal_next - primal) ** 2)
        next_image = row_products(tile_store, primal_next.astype(jnp.bfloat16), blocks)
        dual_state = jnp.maximum(
            dual_state + step_dual * (bounds - (2.0 * next_image - row_image)), 0.0
        )
        violation_part = jnp.sum(jnp.maximum(bounds - next_image, 0.0) ** 2)
        violation = lax.psum(violation_part, ("grp", "dev"))
        weight = jnp.sqrt(weight * jnp.sqrt((violation + 1e-06) / (change + 1e-06)))
        primal = primal_next
        row_image = next_image
    dual_final = lax.all_to_all(
        dual_state[inverse], "dev", split_axis=0, concat_axis=0, tiled=True
    ).reshape(-1)
    return (primal, dual_final, jnp.reshape(weight, (1,)))


MESH_ID = pl.DeviceIdType.MESH
LANES = 128
TILE = 4


def fits(mesh_shape, slots, rows_per, width, blocks, column_blocks):
    n_grp, n_dev = mesh_shape["grp"], mesh_shape["dev"]
    n_chip = n_dev // 2
    if n_dev % 2 or n_chip & (n_chip - 1) or width != n_dev * LANES:
        return False
    if rows_per != LANES or blocks != n_dev or blocks != 8 or slots > 32:
        return False
    if slots % 4 or (n_grp * n_dev * slots) % LANES or column_blocks % LANES:
        return False
    held = slots * rows_per * width * 2 + column_blocks * width * 4 * 5
    return held < 30 * 2**20


def split_kernel(
    n_grp,
    n_dev,
    cols_in,
    counts_in,
    dest_in,
    bounds_in,
    dual_in,
    tiles,
    primal_in,
    cost_in,
    upper_in,
    out_primal,
    out_dual,
    out_weight,
    kv,
    pv,
    cv,
    uv,
    cs,
    us,
    pnow,
    pbf,
    hot,
    hot_back,
    asend,
    abuf,
    bsend,
    bbuf,
    stat,
    fbuf,
    dsend,
    drecv,
    cols_at,
    counts_at,
    dest_at,
    bounds_at,
    dual_at,
    tile_sem,
    local_sem,
    small_sem,
    out_sem,
    a_send,
    a_recv,
    b_send,
    b_recv,
    stat_send,
    stat_recv,
    f_send,
    f_recv,
    p_send,
    p_recv,
    dual_send,
    dual_recv,
):
    slots, rows_per, width = tiles.shape
    blocks = bounds_in.shape[0]
    n_cb = pnow.shape[0]
    n_all = n_grp * n_dev
    n_chip = n_dev // 2
    span = 2 * LANES
    packs = slots // TILE
    f32, bf16, i32 = jnp.float32, jnp.bfloat16, jnp.int32
    g = lax.axis_index("grp")
    d = lax.axis_index("dev")
    core = d % 2
    chip = d // 2
    twin = 1 - core
    partner = chip * 2 + twin
    me = g * n_dev + d

    def remote(src, dst, ssem, rsem, tg, td):
        return pltpu.make_async_remote_copy(
            src_ref=src,
            dst_ref=dst,
            send_sem=ssem,
            recv_sem=rsem,
            device_id={"grp": tg, "dev": td},
            device_id_type=MESH_ID,
        )

    def bytes_of(ref, ssem, rsem):
        return remote(ref, ref, ssem, rsem, g, partner)

    others = [(a, b) for a in range(n_grp) for b in range(n_dev) if a or b]

    def other(a, b):
        return (g + a) % n_grp, (d + b) % n_dev

    def chunk(u):
        return pl.ds(pl.multiple_of((chip ^ u) * span, span), span)

    barrier = pltpu.get_barrier_semaphore()
    for a, b in others:
        tg, td = other(a, b)
        pl.semaphore_signal(
            barrier, inc=1, device_id={"grp": tg, "dev": td}, device_id_type=MESH_ID
        )
    small = [
        pltpu.make_async_copy(src, dst, small_sem.at[k])
        for k, (src, dst) in enumerate(
            (
                (cols_in, cols_at),
                (counts_in, counts_at),
                (dest_in, dest_at),
                (bounds_in, bounds_at),
                (dual_in, dual_at),
            )
        )
    ]
    for copy in small:
        copy.start()
    order = [u for u in range(n_chip - 1, 0, -1)] + [0]
    part = 4
    for u in order:
        for k in range(0, slots, part):
            pltpu.make_async_copy(
                tiles.at[pl.ds(k, part), :, chunk(u)],
                kv.at[pl.ds(k, part), :, chunk(u)],
                tile_sem.at[u],
            ).start()
    copies = [
        pltpu.make_async_copy(primal_in, pv, local_sem.at[0]),
        pltpu.make_async_copy(cost_in, cv, local_sem.at[1]),
        pltpu.make_async_copy(upper_in, uv, local_sem.at[2]),
    ]
    for copy in copies:
        copy.start()

    for copy in small:
        copy.wait()
    cols = [cols_at[k] for k in range(slots)]
    counts = [counts_at[k] for k in range(blocks)]
    dest = [dest_at[k] for k in range(blocks)]
    starts = [counts[0] * 0]
    for b in range(blocks):
        starts.append(starts[-1] + counts[b])
    total = starts[-1]
    live = [jnp.where(s < total, cols[s], -1) for s in range(slots)]
    lane = lax.broadcasted_iota(i32, (1, LANES), 1)
    turn = (me * slots) % LANES
    place = jnp.where(lane < turn, lane - turn + LANES, lane - turn)
    stat_row = jnp.full((1, LANES), -1.0, f32)
    for s in range(slots):
        stat_row = jnp.where(place == s, live[s].astype(f32), stat_row)
    stat[0, me] = stat_row
    rows = 32
    row = lax.broadcasted_iota(i32, (rows, LANES), 0)
    row_owner = jnp.zeros((rows, LANES), i32)
    for b in range(1, blocks):
        row_owner = row_owner + jnp.where(row >= starts[b], 1, 0)
    row_owner = jnp.where(row < total, row_owner, -1)
    own_lane = lax.broadcasted_iota(i32, (blocks, slots), 1)
    own_row = lax.broadcasted_iota(i32, (blocks, slots), 0)
    first = jnp.zeros((blocks, slots), i32)
    last = jnp.zeros((blocks, slots), i32)
    for b in range(blocks):
        first = jnp.where(own_row == b, starts[b], first)
        last = jnp.where(own_row == b, starts[b + 1], last)
    owner_hot = jnp.where((own_lane >= first) & (own_lane < last), 1.0, 0.0).astype(bf16)
    slot_lane = lax.broadcasted_iota(i32, (rows_per, slots), 1)
    bounds = bounds_at[...].astype(f32)
    dual = dual_at[...].astype(f32)

    def pieces(it, dual_now, before):
        spread = jnp.zeros((rows, rows_per), f32)
        for b in range(blocks):
            spread = jnp.where(row_owner == b, dual_now[b : b + 1, :], spread)
        left = [
            jnp.concatenate(
                [jnp.where(row == s, spread, 0.0), jnp.where(row == s + 1, spread, 0.0)],
                axis=1,
            ).astype(bf16)
            for s in range(0, slots, 2)
        ]
        for u in order:
            before(u)
            whole = jnp.zeros((rows, span), f32)
            for s in range(0, slots, 2):
                pair = kv[s : s + 2, :, chunk(u)].reshape(2 * rows_per, span)
                whole = whole + jnp.dot(left[s // 2], pair, preferred_element_type=f32)
            halves = [
                whole[:slots, h * LANES : (h + 1) * LANES].astype(bf16).reshape(packs, TILE, LANES)
                for h in range(2)
            ]
            for h in range(2):
                asend[it, u, h] = halves[h]
            if u == 0:
                abuf[it, pl.ds(me * packs, packs)] = jnp.where(core == 0, halves[0], halves[1])

    def send_pieces(it, u):
        def send(src, tg, td):
            remote(
                src,
                abuf.at[it, pl.ds(me * packs, packs)],
                a_send.at[it],
                a_recv.at[it],
                tg,
                td,
            ).start()

        for a in range(n_grp - 1, 0, -1):
            for h in range(2):
                send(asend.at[it, u, h], (g + a) % n_grp, (chip ^ u) * 2 + h)
        if u:
            for h in range(2):
                send(asend.at[it, u, h], g, (chip ^ u) * 2 + h)
        else:
            send(asend.at[it, 0, twin], g, partner)

    def send_stat(turn_no):
        for a, b in others:
            tg, td = other(a, b)
            remote(
                stat.at[turn_no, me],
                stat.at[turn_no, me],
                stat_send.at[turn_no],
                stat_recv.at[turn_no],
                tg,
                td,
            ).start()

    def stat_bytes(turn_no):
        return bytes_of(
            stat.at[turn_no, pl.ds(0, n_all - 1)], stat_send.at[turn_no], stat_recv.at[turn_no]
        )

    def piece_bytes(it):
        return bytes_of(
            abuf.at[it, pl.ds(0, (n_all - 1) * packs)], a_send.at[it], a_recv.at[it]
        )

    def image_part(acc, picked, lanes):
        for s in range(0, slots, 4):
            block = kv[s : s + 4, :, lanes].reshape(4 * rows_per, span)
            out = lax.dot_general(
                block, picked, (((1,), (1,)), ((), ())), preferred_element_type=f32
            )
            for k in range(4):
                here = out[k * rows_per : (k + 1) * rows_per]
                acc = jnp.where(slot_lane == s + k, acc + here, acc)
        return acc

    def image_of(acc):
        high = acc.astype(bf16)
        rest = acc - high.astype(f32)
        mid = rest.astype(bf16)
        low = (rest - mid.astype(f32)).astype(bf16)
        image = jnp.zeros((blocks, rows_per), f32)
        for term in (high, mid, low):
            image = image + lax.dot_general(
                owner_hot, term, (((1,), (1,)), ((), ())), preferred_element_type=f32
            )
        return image

    def no_image():
        return jnp.zeros((rows_per, slots), f32)

    def first_image():
        copies[0].wait()
        for j in range(n_dev):
            value = pv[pl.ds(j, n_cb, stride=n_dev), :]
            pbf[:, j * LANES : (j + 1) * LANES] = value.astype(bf16)
        pnow[...] = pv[pl.ds(d, n_cb, stride=n_dev), :]
        wide = lax.broadcasted_iota(i32, (rows, n_cb), 0)
        wide_col = jnp.full((rows, n_cb), -1, i32)
        for s in range(slots):
            wide_col = jnp.where(wide == s, live[s], wide_col)
        own_hot = jnp.where(
            wide_col == lax.broadcasted_iota(i32, (rows, n_cb), 1), 1.0, 0.0
        ).astype(bf16)
        picked = jnp.dot(own_hot, pbf[...], preferred_element_type=f32).astype(bf16)[:slots]
        acc = no_image()
        for c in range(n_chip):
            lanes = slice(c * span, (c + 1) * span)
            acc = image_part(acc, picked[:, lanes], lanes)
        return image_of(acc)

    def build_hot():
        stat_bytes(0).wait_recv()
        block_of = lax.broadcasted_iota(i32, (n_cb, LANES), 0).astype(f32)
        for t in range(n_all * slots // LANES):
            line = jnp.full((1, LANES), -1.0, f32)
            for k in range(n_all):
                low, high = k * slots - t * LANES, (k + 1) * slots - t * LANES
                if high > 0 and low < LANES:
                    line = jnp.where((lane >= low) & (lane < high), stat[0, k], line)
            hot[:, t * LANES : (t + 1) * LANES] = jnp.where(block_of == line, 1.0, 0.0).astype(bf16)
        back = n_dev * slots
        back_row = lax.broadcasted_iota(i32, (back, LANES), 0)
        back_lane = lax.broadcasted_iota(i32, (back, LANES), 1)
        back_dev, back_slot = back_row // slots, back_row % slots
        found = jnp.zeros((back, LANES), f32)
        for u in range(n_chip):
            for h in range(2):
                src = g * n_dev + (chip ^ u) * 2 + h
                shift = (src * slots) % LANES
                at = jnp.where(back_lane < shift, back_lane - shift + LANES, back_lane - shift)
                hit = (back_dev == u * 2 + h) & (at == back_slot)
                found = jnp.where(hit, stat[0, src] + 1.0, found)
        wanted = jnp.sum(found, axis=1, keepdims=True) - 1.0
        lane_cb = lax.broadcasted_iota(i32, (back, n_cb), 1).astype(f32)
        hot_back[...] = jnp.where(wanted == lane_cb, 1.0, 0.0).astype(bf16)

    def load_slices():
        copies[1].wait()
        copies[2].wait()
        cs[...] = cv[pl.ds(d, n_cb, stride=n_dev), :]
        us[...] = uv[pl.ds(d, n_cb, stride=n_dev), :]

    weight = jnp.ones((1, 1), f32)
    image = None
    for it in range(ITERS):
        if it == 0:

            def ready(u):
                pltpu.make_async_copy(
                    tiles.at[:, :, chunk(u)], kv.at[:, :, chunk(u)], tile_sem.at[u]
                ).wait()

            pieces(it, dual, ready)
            pl.semaphore_wait(barrier, len(others))
            send_stat(0)
            for u in order:
                send_pieces(it, u)
            image = first_image()
            load_slices()
            build_hot()
        else:
            sent_before = []

            def flow(u):
                if sent_before:
                    send_pieces(it, sent_before[-1])
                sent_before.append(u)

            pieces(it, dual, flow)
            send_pieces(it, sent_before[-1])
            stat_bytes(it).wait_recv()
            violation = jnp.sum(stat[it], axis=0)[:, LANES - 1 :]
            change = jnp.sum(stat[it, 0:n_dev], axis=0)[:, :1]
            weight = jnp.sqrt(weight * jnp.sqrt((violation + 1e-06) / (change + 1e-06)))
        tau = step_scale / weight
        piece_bytes(it).wait_recv()
        grad = jnp.dot(
            hot[...],
            abuf.at[it].reshape(n_all * slots, LANES)[...],
            preferred_element_type=f32,
        )
        old = pnow[...]
        new = jnp.minimum(jnp.maximum(old - tau * (cs[...] - grad), 0.0), us[...])
        back = jnp.dot(hot_back[...], new.astype(bf16), preferred_element_type=f32)
        back = back.astype(bf16).reshape(n_chip, 2, packs, TILE, LANES)
        bsend[it] = back
        bbuf[it, 0, core] = jnp.where(core == 0, back[0, 0], back[0, 1])

        def send_back(src, dst, u, td):
            remote(src, dst, b_send.at[it], b_recv.at[it, u], g, td).start()

        for u in order[:-1]:
            for h in range(2):
                send_back(
                    bsend.at[it, u, h], bbuf.at[it, u, core], u, (chip ^ u) * 2 + h
                )
        send_back(bsend.at[it, 0, twin], bbuf.at[it, 0, core], 0, partner)
        gap = new - old
        moved = jnp.sum(gap * gap, axis=(0, 1), keepdims=True)
        if it < ITERS - 1:
            pnow[...] = new
        else:
            fbuf[0] = new
            for u in order[:-1]:
                remote(
                    fbuf.at[0], fbuf.at[u], f_send.at[0], f_recv.at[u], g, (chip ^ u) * 2 + core
                ).start()
            remote(fbuf.at[0], out_primal.at[d], p_send.at[0], p_recv.at[0], g, partner).start()
            pltpu.make_async_copy(fbuf.at[0], out_primal.at[d], out_sem.at[0]).start()

        acc = no_image()
        for u in range(n_chip):
            one = bbuf.at[it, 0, 0] if u == 0 else bbuf.at[it, u]
            bytes_of(one, b_send.at[it], b_recv.at[it, u]).wait_recv()
            picked = jnp.concatenate(
                [bbuf[it, u, h].reshape(slots, LANES) for h in range(2)], axis=1
            )
            acc = image_part(acc, picked, chunk(u))
        next_image = image_of(acc)
        sigma = step_scale * weight
        dual = jnp.maximum(dual + sigma * (bounds - (2.0 * next_image - image)), 0.0)
        short = jnp.maximum(bounds - next_image, 0.0)
        image = next_image
        missed = jnp.sum(short * short, axis=(0, 1), keepdims=True)
        stat[it + 1, me] = jnp.where(lane < LANES // 2, moved, missed)
        send_stat(it + 1)

    for e in range(n_dev):
        line = jnp.zeros((1, rows_per), f32)
        for k in range(blocks):
            line = jnp.where(dest[k] == e, dual[k : k + 1, :], line)
        dsend[e] = line
    for k in range(1, n_dev):
        td = (d + k) % n_dev
        remote(dsend.at[td], drecv.at[d], dual_send.at[0], dual_recv.at[0], g, td).start()
    drecv[d] = dsend[d]
    for u in range(1, n_chip):
        bytes_of(fbuf.at[u], f_send.at[0], f_recv.at[u]).wait_recv()
        src = (chip ^ u) * 2 + core
        remote(fbuf.at[u], out_primal.at[src], p_send.at[0], p_recv.at[0], g, partner).start()
        pltpu.make_async_copy(fbuf.at[u], out_primal.at[src], out_sem.at[0]).start()
    bytes_of(drecv.at[pl.ds(0, n_dev - 1)], dual_send.at[0], dual_recv.at[0]).wait_recv()
    out_dual[...] = drecv[...]
    stat_bytes(ITERS).wait_recv()
    violation = jnp.sum(stat[ITERS], axis=0)[:, LANES - 1 :]
    change = jnp.sum(stat[ITERS, 0:n_dev], axis=0)[:, :1]
    weight = jnp.sqrt(weight * jnp.sqrt((violation + 1e-06) / (change + 1e-06)))
    out_weight[...] = jnp.broadcast_to(weight, (1, LANES))
    for it in range(ITERS):
        piece_bytes(it).wait_send()
        bytes_of(
            bbuf.at[it, pl.ds(0, n_chip - 1)], b_send.at[it], b_recv.at[it, 0]
        ).wait_send()
        bytes_of(bbuf.at[it, 0, 0], b_send.at[it], b_recv.at[it, 0]).wait_send()
    for turn_no in range(ITERS + 1):
        stat_bytes(turn_no).wait_send()
    bytes_of(drecv.at[pl.ds(0, n_dev - 1)], dual_send.at[0], dual_recv.at[0]).wait_send()
    bytes_of(fbuf.at[pl.ds(0, n_chip - 1)], f_send.at[0], f_recv.at[0]).wait_send()
    bytes_of(fbuf, p_send.at[0], p_recv.at[0]).wait_send()
    bytes_of(fbuf, p_send.at[0], p_recv.at[0]).wait_recv()
    pltpu.make_async_copy(fbuf, out_primal.at[pl.ds(0, n_chip)], out_sem.at[0]).wait()


def split_device(mesh_shape, *args):
    tiles, cols, counts, dest, row_bounds, dual_start, primal, cost, upper = args
    slots, rows_per, width = tiles.shape
    blocks = counts.shape[0]
    n_cb = primal.shape[0] // width
    if not fits(mesh_shape, slots, rows_per, width, blocks, n_cb):
        return per_device(*args)
    n_grp, n_dev = mesh_shape["grp"], mesh_shape["dev"]
    n_all, n_chip = n_grp * n_dev, n_dev // 2
    packs = slots // TILE
    flat = (primal.shape[0] // LANES, LANES)
    f32, bf16 = jnp.float32, jnp.bfloat16
    vmem = pl.BlockSpec(memory_space=pltpu.VMEM)
    far = pl.BlockSpec(memory_space=pltpu.HBM)
    dma = pltpu.SemaphoreType.DMA
    out_primal, out_dual, out_weight = pl.pallas_call(
        functools.partial(split_kernel, n_grp, n_dev),
        name="pdhg_split",
        out_shape=(
            jax.ShapeDtypeStruct((n_dev, n_cb, LANES), f32),
            jax.ShapeDtypeStruct((n_dev, 1, rows_per), f32),
            jax.ShapeDtypeStruct((1, LANES), f32),
        ),
        in_specs=[far] * 9,
        out_specs=(far, vmem, vmem),
        scratch_shapes=[
            pltpu.VMEM((slots, rows_per, width), bf16),
            pltpu.VMEM(flat, f32),
            pltpu.VMEM(flat, f32),
            pltpu.VMEM(flat, f32),
            pltpu.VMEM((n_cb, LANES), f32),
            pltpu.VMEM((n_cb, LANES), f32),
            pltpu.VMEM((n_cb, LANES), f32),
            pltpu.VMEM((n_cb, width), bf16),
            pltpu.VMEM((n_cb, n_all * slots), bf16),
            pltpu.VMEM((n_dev * slots, n_cb), bf16),
            pltpu.VMEM((ITERS, n_chip, 2, packs, TILE, LANES), bf16),
            pltpu.VMEM((ITERS, n_all * packs, TILE, LANES), bf16),
            pltpu.VMEM((ITERS, n_chip, 2, packs, TILE, LANES), bf16),
            pltpu.VMEM((ITERS, n_chip, 2, packs, TILE, LANES), bf16),
            pltpu.VMEM((ITERS + 1, n_all, 1, LANES), f32),
            pltpu.VMEM((n_chip, n_cb, LANES), f32),
            pltpu.VMEM((n_dev, 1, rows_per), f32),
            pltpu.VMEM((n_dev, 1, rows_per), f32),
            pltpu.SMEM((slots,), jnp.int32),
            pltpu.SMEM((blocks,), jnp.int32),
            pltpu.SMEM((blocks,), jnp.int32),
            pltpu.VMEM((blocks, rows_per), bf16),
            pltpu.VMEM((blocks, rows_per), bf16),
            dma((n_chip,)),
            dma((3,)),
            dma((5,)),
            dma((1,)),
            dma((ITERS,)),
            dma((ITERS,)),
            dma((ITERS,)),
            dma((ITERS, n_chip)),
            dma((ITERS + 1,)),
            dma((ITERS + 1,)),
            dma((1,)),
            dma((n_chip,)),
            dma((1,)),
            dma((1,)),
            dma((1,)),
            dma((1,)),
        ],
        compiler_params=pltpu.CompilerParams(
            collective_id=0, has_side_effects=True, vmem_limit_bytes=65 * 10**6
        ),
    )(
        cols,
        counts,
        dest,
        row_bounds.reshape(blocks, rows_per),
        dual_start.reshape(blocks, rows_per),
        tiles,
        primal.reshape(flat),
        cost.reshape(flat),
        upper.reshape(flat),
    )
    primal_final = out_primal.transpose(1, 0, 2).reshape(-1)
    return primal_final, out_dual.reshape(-1), out_weight[0, :1]


def solution(mesh):
    in_specs = (
        P(("grp", "dev"), None, None),
        P(("grp", "dev")),
        P(("grp", "dev")),
        P(("grp", "dev")),
        P(("grp", "dev")),
        P(("grp", "dev")),
        P(),
        P(),
        P(),
    )
    out_specs = (P(), P(("grp", "dev")), P())
    return jax.shard_map(
        functools.partial(split_device, dict(mesh.shape)),
        mesh=mesh,
        in_specs=in_specs,
        out_specs=out_specs,
        check_vma=False,
    )
```

```python
import functools

import jax
import jax.numpy as jnp
from jax import lax
from jax.experimental import pallas as pl
from jax.experimental.pallas import tpu as pltpu
from jax.sharding import PartitionSpec as P

NCB = 256
ITERS = 3


step_scale = 0.3


def row_products(tile_store, vector_bf, blocks):
    tile_set, tile_cols, owners, live_flags = tile_store
    vector_table = vector_bf.reshape(-1, tile_set.shape[2])
    column_hot = (
        tile_cols[:, None] == jnp.arange(vector_table.shape[0], dtype=jnp.int32)[None, :]
    ).astype(jnp.bfloat16)
    picked = jnp.dot(column_hot, vector_table, preferred_element_type=jnp.float32).astype(
        jnp.bfloat16
    )
    product = jnp.einsum("src,sc->sr", tile_set, picked, preferred_element_type=jnp.float32)
    product = jnp.where(live_flags[:, None], product, 0.0)
    owner_hot = (jnp.arange(blocks, dtype=jnp.int32)[:, None] == owners[None, :]).astype(
        jnp.float32
    )
    return jnp.dot(owner_hot, product, precision=lax.Precision.HIGHEST)


def column_products(tile_store, rows_bf):
    tile_set, tile_cols, owners, live_flags = tile_store
    blocks = rows_bf.shape[0]
    owner_hot = (owners[:, None] == jnp.arange(blocks, dtype=jnp.int32)[None, :]).astype(
        jnp.bfloat16
    )
    picked_rows = jnp.dot(owner_hot, rows_bf, preferred_element_type=jnp.float32).astype(
        jnp.bfloat16
    )
    product = jnp.einsum("src,sr->sc", tile_set, picked_rows, preferred_element_type=jnp.float32)
    product = jnp.where(live_flags[:, None], product, 0.0)
    column_hot = (jnp.arange(NCB, dtype=jnp.int32)[:, None] == tile_cols[None, :]).astype(
        jnp.float32
    )
    return jnp.dot(column_hot, product, precision=lax.Precision.HIGHEST).reshape(-1)


def per_device(
    matrix_tiles,
    tile_column,
    block_counts,
    destination,
    row_bounds,
    dual_start,
    primal_start,
    cost_vector,
    upper_bound,
):
    blocks = block_counts.shape[0]
    rows_per = matrix_tiles.shape[1]
    slot_count = matrix_tiles.shape[0]
    starts = jnp.cumsum(block_counts) - block_counts
    slot_ids = jnp.arange(slot_count, dtype=jnp.int32)
    owners = jnp.sum((starts[None, 1:] <= slot_ids[:, None]).astype(jnp.int32), axis=1)
    bounds_here = row_bounds.reshape(blocks, rows_per)
    dual_here = dual_start.reshape(blocks, rows_per)
    peer_ids = jnp.arange(blocks, dtype=jnp.int32)
    inverse = jnp.sum(
        jnp.where(destination[None, :] == peer_ids[:, None], peer_ids[None, :], 0), axis=1
    )
    tile_store = (matrix_tiles, tile_column, owners, slot_ids < jnp.sum(block_counts))
    bounds = bounds_here.astype(jnp.float32)
    dual_state = dual_here.astype(jnp.float32)
    primal = primal_start
    weight = jnp.ones((), jnp.float32)
    row_image = row_products(tile_store, primal.astype(jnp.bfloat16), blocks)
    for iteration in range(ITERS):
        step_primal = step_scale / weight
        step_dual = step_scale * weight
        partial_value = column_products(tile_store, dual_state.astype(jnp.bfloat16))
        gradient = lax.psum(partial_value, ("grp", "dev"))
        primal_next = jnp.clip(primal - step_primal * (cost_vector - gradient), 0.0, upper_bound)
        change = jnp.sum((primal_next - primal) ** 2)
        next_image = row_products(tile_store, primal_next.astype(jnp.bfloat16), blocks)
        dual_state = jnp.maximum(
            dual_state + step_dual * (bounds - (2.0 * next_image - row_image)), 0.0
        )
        violation_part = jnp.sum(jnp.maximum(bounds - next_image, 0.0) ** 2)
        violation = lax.psum(violation_part, ("grp", "dev"))
        weight = jnp.sqrt(weight * jnp.sqrt((violation + 1e-06) / (change + 1e-06)))
        primal = primal_next
        row_image = next_image
    dual_final = lax.all_to_all(
        dual_state[inverse], "dev", split_axis=0, concat_axis=0, tiled=True
    ).reshape(-1)
    return (primal, dual_final, jnp.reshape(weight, (1,)))


MESH_ID = pl.DeviceIdType.MESH
LANES = 128
TILE = 4


def fits(mesh_shape, slots, rows_per, width, blocks, column_blocks):
    n_grp, n_dev = mesh_shape["grp"], mesh_shape["dev"]
    n_chip = n_dev // 2
    if n_dev % 2 or n_chip & (n_chip - 1) or n_grp & (n_grp - 1) or width != n_dev * LANES:
        return False
    if rows_per != LANES or blocks != n_dev or blocks != 8 or slots > 32:
        return False
    if slots % 4 or (n_grp * n_dev * slots) % LANES or column_blocks % LANES:
        return False
    held = slots * rows_per * width * 2 + column_blocks * width * 4 * 5
    return held < 30 * 2**20


def split_kernel(
    n_grp,
    n_dev,
    cols_in,
    counts_in,
    dest_in,
    bounds_in,
    dual_in,
    tiles,
    primal_in,
    cost_in,
    upper_in,
    out_primal,
    out_dual,
    out_weight,
    kv,
    pv,
    cv,
    uv,
    cs,
    us,
    pnow,
    pbf,
    hot,
    hot_back,
    asend,
    abuf,
    bsend,
    bbuf,
    stat,
    dsend,
    drecv,
    cols_at,
    counts_at,
    dest_at,
    bounds_at,
    dual_at,
    tile_sem,
    local_sem,
    small_sem,
    a_send,
    a_recv,
    b_send,
    b_recv,
    stat_send,
    stat_recv,
    f_send,
    f_recv,
    p_send,
    p_recv,
    dual_send,
    dual_recv,
):
    slots, rows_per, width = tiles.shape
    blocks = bounds_in.shape[0]
    n_cb = pnow.shape[0]
    n_all = n_grp * n_dev
    n_chip = n_dev // 2
    span = 2 * LANES
    packs = slots // TILE
    f32, bf16, i32 = jnp.float32, jnp.bfloat16, jnp.int32
    g = lax.axis_index("grp")
    d = lax.axis_index("dev")
    core = d % 2
    chip = d // 2
    twin = 1 - core
    partner = chip * 2 + twin
    me = g * n_dev + d

    def remote(src, dst, ssem, rsem, tg, td):
        return pltpu.make_async_remote_copy(
            src_ref=src,
            dst_ref=dst,
            send_sem=ssem,
            recv_sem=rsem,
            device_id={"grp": tg, "dev": td},
            device_id_type=MESH_ID,
        )

    def bytes_of(ref, ssem, rsem):
        return remote(ref, ref, ssem, rsem, g, partner)

    others = [(a, b) for a in range(n_grp) for b in range(n_dev) if a or b]

    def other(a, b):
        return (g + a) % n_grp, (d + b) % n_dev

    def chunk(u):
        return pl.ds(pl.multiple_of((chip ^ u) * span, span), span)

    barrier = pltpu.get_barrier_semaphore()
    for a, b in others:
        tg, td = other(a, b)
        pl.semaphore_signal(
            barrier, inc=1, device_id={"grp": tg, "dev": td}, device_id_type=MESH_ID
        )
    small = [
        pltpu.make_async_copy(src, dst, small_sem.at[k])
        for k, (src, dst) in enumerate(
            (
                (cols_in, cols_at),
                (counts_in, counts_at),
                (dest_in, dest_at),
                (bounds_in, bounds_at),
                (dual_in, dual_at),
            )
        )
    ]
    for copy in small:
        copy.start()
    order = [u for u in range(n_chip - 1, 0, -1)] + [0]
    planes = sorted(range(1, n_grp), key=lambda a: (-(a.bit_length()), a))
    part = 4
    group = slots // 4

    def fetch(u):
        for k in range(0, slots, part):
            pltpu.make_async_copy(
                tiles.at[pl.ds(k, part), :, chunk(u)],
                kv.at[pl.ds(k, part), :, chunk(u)],
                tile_sem.at[u],
            ).start()

    fetch(order[0])
    copies = [
        pltpu.make_async_copy(primal_in, pv, local_sem.at[0]),
        pltpu.make_async_copy(cost_in, cv, local_sem.at[1]),
        pltpu.make_async_copy(upper_in, uv, local_sem.at[2]),
    ]

    for copy in small:
        copy.wait()
    for u in order[1:]:
        fetch(u)
    cols = [cols_at[k] for k in range(slots)]
    counts = [counts_at[k] for k in range(blocks)]
    dest = [dest_at[k] for k in range(blocks)]
    starts = [counts[0] * 0]
    for b in range(blocks):
        starts.append(starts[-1] + counts[b])
    total = starts[-1]
    live = [jnp.where(s < total, cols[s], -1) for s in range(slots)]
    lane = lax.broadcasted_iota(i32, (1, LANES), 1)
    turn = (me * slots) % LANES
    place = jnp.where(lane < turn, lane - turn + LANES, lane - turn)
    stat_row = jnp.full((1, LANES), -1.0, f32)
    for s in range(slots):
        stat_row = jnp.where(place == s, live[s].astype(f32), stat_row)
    stat[0, me] = stat_row
    rows = 16
    row = lax.broadcasted_iota(i32, (rows, LANES), 0)
    split = (slots // 2 + 1) // 2 * 2
    lead = split % TILE
    groups = []
    for low, high, base in ((0, split, 0), (split, slots, split - lead)):
        slot = row + base
        owner = jnp.zeros((rows, LANES), i32)
        for b in range(1, blocks):
            owner = owner + jnp.where(slot >= starts[b], 1, 0)
        owner = jnp.where((slot < total) & (slot >= low) & (slot < high), owner, -1)
        groups.append((low, high, slot, owner))
    own_lane = lax.broadcasted_iota(i32, (blocks, slots), 1)
    own_row = lax.broadcasted_iota(i32, (blocks, slots), 0)
    first = jnp.zeros((blocks, slots), i32)
    last = jnp.zeros((blocks, slots), i32)
    for b in range(blocks):
        first = jnp.where(own_row == b, starts[b], first)
        last = jnp.where(own_row == b, starts[b + 1], last)
    owner_hot = jnp.where((own_lane >= first) & (own_lane < last), 1.0, 0.0).astype(bf16)
    slot_lane = lax.broadcasted_iota(i32, (rows_per, slots), 1)
    bounds = bounds_at[...].astype(f32)
    dual = dual_at[...].astype(f32)

    def pieces(it, dual_now, before):
        left = {}
        for low, high, slot, owner in groups:
            spread = jnp.zeros((rows, rows_per), f32)
            for b in range(blocks):
                spread = jnp.where(owner == b, dual_now[b : b + 1, :], spread)
            for s in range(low, high, 2):
                left[s] = jnp.concatenate(
                    [jnp.where(slot == s, spread, 0.0), jnp.where(slot == s + 1, spread, 0.0)],
                    axis=1,
                ).astype(bf16)
        for u in order:
            before(u)
            sums = []
            for low, high, _, _ in groups:
                whole = jnp.zeros((rows, span), f32)
                for s in range(low, high, 2):
                    pair = kv[s : s + 2, :, chunk(u)].reshape(2 * rows_per, span)
                    whole = whole + jnp.dot(left[s], pair, preferred_element_type=f32)
                sums.append(whole)
            head, tail = sums[0], sums[1]
            even = split - lead
            joined = [head[:even]]
            if lead:
                joined.append(head[even : even + TILE] + tail[:TILE])
                joined.append(tail[TILE : slots - even])
            else:
                joined.append(tail[: slots - even])
            halves = [
                [
                    x[:, h * LANES : (h + 1) * LANES].astype(bf16).reshape(-1, TILE, LANES)
                    for x in joined
                ]
                for h in range(2)
            ]
            halves = [jnp.concatenate(x, axis=0) for x in halves]
            for h in range(2):
                asend[it, u, h] = halves[h]
            if u == 0:
                abuf[it, pl.ds(me * packs, packs)] = jnp.where(core == 0, halves[0], halves[1])

    def send_pieces(it, u):
        def send(src, tg, td):
            remote(
                src,
                abuf.at[it, pl.ds(me * packs, packs)],
                a_send.at[it],
                a_recv.at[it],
                tg,
                td,
            ).start()

        for a in planes:
            for h in range(2):
                send(asend.at[it, u, h], g ^ a, (chip ^ u) * 2 + h)
        if u:
            for h in range(2):
                send(asend.at[it, u, h], g, (chip ^ u) * 2 + h)
        else:
            send(asend.at[it, 0, twin], g, partner)

    def send_stat(turn_no):
        for a, b in others:
            tg, td = other(a, b)
            remote(
                stat.at[turn_no, me],
                stat.at[turn_no, me],
                stat_send.at[turn_no],
                stat_recv.at[turn_no],
                tg,
                td,
            ).start()

    def stat_bytes(turn_no):
        return bytes_of(
            stat.at[turn_no, pl.ds(0, n_all - 1)], stat_send.at[turn_no], stat_recv.at[turn_no]
        )

    def piece_bytes(it):
        return bytes_of(
            abuf.at[it, pl.ds(0, (n_all - 1) * packs)], a_send.at[it], a_recv.at[it]
        )

    def image_part(acc, picked, lanes):
        for s in range(0, slots, group):
            block = kv[s : s + group, :, lanes].reshape(group * rows_per, span)
            out = lax.dot_general(
                block, picked, (((1,), (1,)), ((), ())), preferred_element_type=f32
            )
            for k in range(group):
                here = out[k * rows_per : (k + 1) * rows_per]
                acc = jnp.where(slot_lane == s + k, acc + here, acc)
        return acc

    def image_of(acc):
        high = acc.astype(bf16)
        rest = acc - high.astype(f32)
        mid = rest.astype(bf16)
        low = (rest - mid.astype(f32)).astype(bf16)
        image = jnp.zeros((blocks, rows_per), f32)
        for term in (high, mid, low):
            image = image + lax.dot_general(
                owner_hot, term, (((1,), (1,)), ((), ())), preferred_element_type=f32
            )
        return image

    def no_image():
        return jnp.zeros((rows_per, slots), f32)

    def first_image():
        copies[0].wait()
        for j in range(n_dev):
            value = pv[pl.ds(j, n_cb, stride=n_dev), :]
            pbf[:, j * LANES : (j + 1) * LANES] = value.astype(bf16)
        pnow[...] = pv[pl.ds(d, n_cb, stride=n_dev), :]
        wide = lax.broadcasted_iota(i32, (32, n_cb), 0)
        wide_col = jnp.full((32, n_cb), -1, i32)
        for s in range(slots):
            wide_col = jnp.where(wide == s, live[s], wide_col)
        own_hot = jnp.where(
            wide_col == lax.broadcasted_iota(i32, (32, n_cb), 1), 1.0, 0.0
        ).astype(bf16)
        picked = jnp.dot(own_hot, pbf[...], preferred_element_type=f32).astype(bf16)[:slots]
        acc = no_image()
        for c in range(n_chip):
            lanes = slice(c * span, (c + 1) * span)
            acc = image_part(acc, picked[:, lanes], lanes)
        return image_of(acc)

    def build_hot():
        stat_bytes(0).wait_recv()
        block_of = lax.broadcasted_iota(i32, (n_cb, LANES), 0).astype(f32)
        for t in range(n_all * slots // LANES):
            line = jnp.full((1, LANES), -1.0, f32)
            for k in range(n_all):
                low, high = k * slots - t * LANES, (k + 1) * slots - t * LANES
                if high > 0 and low < LANES:
                    line = jnp.where((lane >= low) & (lane < high), stat[0, k], line)
            hot[:, t * LANES : (t + 1) * LANES] = jnp.where(block_of == line, 1.0, 0.0).astype(bf16)
        back = n_dev * slots
        back_row = lax.broadcasted_iota(i32, (back, LANES), 0)
        back_lane = lax.broadcasted_iota(i32, (back, LANES), 1)
        back_dev, back_slot = back_row // slots, back_row % slots
        found = jnp.zeros((back, LANES), f32)
        for u in range(n_chip):
            for h in range(2):
                src = g * n_dev + (chip ^ u) * 2 + h
                shift = (src * slots) % LANES
                at = jnp.where(back_lane < shift, back_lane - shift + LANES, back_lane - shift)
                hit = (back_dev == u * 2 + h) & (at == back_slot)
                found = jnp.where(hit, stat[0, src] + 1.0, found)
        wanted = jnp.sum(found, axis=1, keepdims=True) - 1.0
        lane_cb = lax.broadcasted_iota(i32, (back, n_cb), 1).astype(f32)
        hot_back[...] = jnp.where(wanted == lane_cb, 1.0, 0.0).astype(bf16)

    def load_slices():
        copies[1].wait()
        copies[2].wait()
        cs[...] = cv[pl.ds(d, n_cb, stride=n_dev), :]
        us[...] = uv[pl.ds(d, n_cb, stride=n_dev), :]

    weight = jnp.ones((1, 1), f32)
    image = None
    for it in range(ITERS):
        if it == 0:

            def ready(u):
                if u == order[-1]:
                    for copy in copies:
                        copy.start()
                pltpu.make_async_copy(
                    tiles.at[:, :, chunk(u)], kv.at[:, :, chunk(u)], tile_sem.at[u]
                ).wait()

            pieces(it, dual, ready)
            pl.semaphore_wait(barrier, len(others))
            send_stat(0)
            for u in order:
                send_pieces(it, u)
            image = first_image()
            load_slices()
            build_hot()
        else:
            sent_before = []

            def flow(u):
                if sent_before:
                    send_pieces(it, sent_before[-1])
                sent_before.append(u)

            pieces(it, dual, flow)
            send_pieces(it, sent_before[-1])
            stat_bytes(it).wait_recv()
            violation = jnp.sum(stat[it], axis=0)[:, LANES - 1 :]
            change = jnp.sum(stat[it, 0:n_dev], axis=0)[:, :1]
            weight = jnp.sqrt(weight * jnp.sqrt((violation + 1e-06) / (change + 1e-06)))
        tau = step_scale / weight
        piece_bytes(it).wait_recv()
        grad = jnp.dot(
            hot[...],
            abuf.at[it].reshape(n_all * slots, LANES)[...],
            preferred_element_type=f32,
        )
        old = pnow[...]
        new = jnp.minimum(jnp.maximum(old - tau * (cs[...] - grad), 0.0), us[...])
        back = jnp.dot(hot_back[...], new.astype(bf16), preferred_element_type=f32)
        back = back.astype(bf16).reshape(n_chip, 2, packs, TILE, LANES)
        bsend[it] = back
        bbuf[it, 0, core] = jnp.where(core == 0, back[0, 0], back[0, 1])

        def send_back(src, dst, u, td):
            remote(src, dst, b_send.at[it], b_recv.at[it, u], g, td).start()

        for u in order[:-1]:
            for h in range(2):
                send_back(
                    bsend.at[it, u, h], bbuf.at[it, u, core], u, (chip ^ u) * 2 + h
                )
        send_back(bsend.at[it, 0, twin], bbuf.at[it, 0, core], 0, partner)
        gap = new - old
        moved = jnp.sum(gap * gap, axis=(0, 1), keepdims=True)
        if it < ITERS - 1:
            pnow[...] = new
        else:
            out_primal[d] = new
            for u in order[:-1]:
                remote(
                    out_primal.at[d],
                    out_primal.at[d],
                    f_send.at[0],
                    f_recv.at[u],
                    g,
                    (chip ^ u) * 2 + core,
                ).start()
            remote(
                out_primal.at[d], out_primal.at[d], p_send.at[0], p_recv.at[0], g, partner
            ).start()

        acc = no_image()
        for u in range(n_chip):
            one = bbuf.at[it, 0, 0] if u == 0 else bbuf.at[it, u]
            bytes_of(one, b_send.at[it], b_recv.at[it, u]).wait_recv()
            picked = jnp.concatenate(
                [bbuf[it, u, h].reshape(slots, LANES) for h in range(2)], axis=1
            )
            acc = image_part(acc, picked, chunk(u))
        next_image = image_of(acc)
        sigma = step_scale * weight
        dual = jnp.maximum(dual + sigma * (bounds - (2.0 * next_image - image)), 0.0)
        short = jnp.maximum(bounds - next_image, 0.0)
        image = next_image
        missed = jnp.sum(short * short, axis=(0, 1), keepdims=True)
        stat[it + 1, me] = jnp.where(lane < LANES // 2, moved, missed)
        send_stat(it + 1)

    for e in range(n_dev):
        line = jnp.zeros((1, rows_per), f32)
        for k in range(blocks):
            line = jnp.where(dest[k] == e, dual[k : k + 1, :], line)
        dsend[e] = line
    for k in range(1, n_dev):
        td = (d + k) % n_dev
        remote(dsend.at[td], drecv.at[d], dual_send.at[0], dual_recv.at[0], g, td).start()
    drecv[d] = dsend[d]
    for u in range(1, n_chip):
        src = (chip ^ u) * 2 + core
        bytes_of(out_primal.at[src], f_send.at[0], f_recv.at[u]).wait_recv()
        remote(
            out_primal.at[src], out_primal.at[src], p_send.at[0], p_recv.at[0], g, partner
        ).start()
    bytes_of(drecv.at[pl.ds(0, n_dev - 1)], dual_send.at[0], dual_recv.at[0]).wait_recv()
    out_dual[...] = drecv[...]
    stat_bytes(ITERS).wait_recv()
    violation = jnp.sum(stat[ITERS], axis=0)[:, LANES - 1 :]
    change = jnp.sum(stat[ITERS, 0:n_dev], axis=0)[:, :1]
    weight = jnp.sqrt(weight * jnp.sqrt((violation + 1e-06) / (change + 1e-06)))
    out_weight[...] = jnp.broadcast_to(weight, (1, LANES))
    for it in range(ITERS):
        piece_bytes(it).wait_send()
        bytes_of(
            bbuf.at[it, pl.ds(0, n_chip - 1)], b_send.at[it], b_recv.at[it, 0]
        ).wait_send()
        bytes_of(bbuf.at[it, 0, 0], b_send.at[it], b_recv.at[it, 0]).wait_send()
    for turn_no in range(ITERS + 1):
        stat_bytes(turn_no).wait_send()
    bytes_of(drecv.at[pl.ds(0, n_dev - 1)], dual_send.at[0], dual_recv.at[0]).wait_send()
    bytes_of(out_primal.at[pl.ds(0, n_chip - 1)], f_send.at[0], f_recv.at[0]).wait_send()
    bytes_of(out_primal.at[pl.ds(0, n_chip)], p_send.at[0], p_recv.at[0]).wait_send()
    bytes_of(out_primal.at[pl.ds(0, n_chip)], p_send.at[0], p_recv.at[0]).wait_recv()


def split_device(mesh_shape, *args):
    tiles, cols, counts, dest, row_bounds, dual_start, primal, cost, upper = args
    slots, rows_per, width = tiles.shape
    blocks = counts.shape[0]
    n_cb = primal.shape[0] // width
    if not fits(mesh_shape, slots, rows_per, width, blocks, n_cb):
        return per_device(*args)
    n_grp, n_dev = mesh_shape["grp"], mesh_shape["dev"]
    n_all, n_chip = n_grp * n_dev, n_dev // 2
    packs = slots // TILE
    flat = (primal.shape[0] // LANES, LANES)
    f32, bf16 = jnp.float32, jnp.bfloat16
    vmem = pl.BlockSpec(memory_space=pltpu.VMEM)
    far = pl.BlockSpec(memory_space=pltpu.HBM)
    dma = pltpu.SemaphoreType.DMA
    out_primal, out_dual, out_weight = pl.pallas_call(
        functools.partial(split_kernel, n_grp, n_dev),
        name="pdhg_split",
        out_shape=(
            pltpu.VMEM((n_dev, n_cb, LANES), f32),
            pltpu.VMEM((n_dev, 1, rows_per), f32),
            pltpu.VMEM((1, LANES), f32),
        ),
        in_specs=[far] * 9,
        out_specs=(vmem, vmem, vmem),
        scratch_shapes=[
            pltpu.VMEM((slots, rows_per, width), bf16),
            pltpu.VMEM(flat, f32),
            pltpu.VMEM(flat, f32),
            pltpu.VMEM(flat, f32),
            pltpu.VMEM((n_cb, LANES), f32),
            pltpu.VMEM((n_cb, LANES), f32),
            pltpu.VMEM((n_cb, LANES), f32),
            pltpu.VMEM((n_cb, width), bf16),
            pltpu.VMEM((n_cb, n_all * slots), bf16),
            pltpu.VMEM((n_dev * slots, n_cb), bf16),
            pltpu.VMEM((ITERS, n_chip, 2, packs, TILE, LANES), bf16),
            pltpu.VMEM((ITERS, n_all * packs, TILE, LANES), bf16),
            pltpu.VMEM((ITERS, n_chip, 2, packs, TILE, LANES), bf16),
            pltpu.VMEM((ITERS, n_chip, 2, packs, TILE, LANES), bf16),
            pltpu.VMEM((ITERS + 1, n_all, 1, LANES), f32),
            pltpu.VMEM((n_dev, 1, rows_per), f32),
            pltpu.VMEM((n_dev, 1, rows_per), f32),
            pltpu.SMEM((slots,), jnp.int32),
            pltpu.SMEM((blocks,), jnp.int32),
            pltpu.SMEM((blocks,), jnp.int32),
            pltpu.VMEM((blocks, rows_per), bf16),
            pltpu.VMEM((blocks, rows_per), bf16),
            dma((n_chip,)),
            dma((3,)),
            dma((5,)),
            dma((ITERS,)),
            dma((ITERS,)),
            dma((ITERS,)),
            dma((ITERS, n_chip)),
            dma((ITERS + 1,)),
            dma((ITERS + 1,)),
            dma((1,)),
            dma((n_chip,)),
            dma((1,)),
            dma((1,)),
            dma((1,)),
            dma((1,)),
        ],
        compiler_params=pltpu.CompilerParams(
            collective_id=0, has_side_effects=True, vmem_limit_bytes=65 * 10**6
        ),
    )(
        *(
            pltpu.with_memory_space_constraint(x, pltpu.HBM)
            for x in (
                cols,
                counts,
                dest,
                row_bounds.reshape(blocks, rows_per),
                dual_start.reshape(blocks, rows_per),
                tiles,
                primal.reshape(flat),
                cost.reshape(flat),
                upper.reshape(flat),
            )
        )
    )
    primal_final = out_primal.transpose(1, 0, 2).reshape(-1)
    return primal_final, out_dual.reshape(-1), out_weight[0, :1]


def solution(mesh):
    in_specs = (
        P(("grp", "dev"), None, None),
        P(("grp", "dev")),
        P(("grp", "dev")),
        P(("grp", "dev")),
        P(("grp", "dev")),
        P(("grp", "dev")),
        P(),
        P(),
        P(),
    )
    out_specs = (P(), P(("grp", "dev")), P())
    return jax.shard_map(
        functools.partial(split_device, dict(mesh.shape)),
        mesh=mesh,
        in_specs=in_specs,
        out_specs=out_specs,
        check_vma=False,
    )
```

```python
import functools

import jax
import jax.numpy as jnp
from jax import lax
from jax.experimental import pallas as pl
from jax.experimental.pallas import tpu as pltpu
from jax.sharding import PartitionSpec as P

NCB = 256
ITERS = 3


step_scale = 0.3


def row_products(tile_store, vector_bf, blocks):
    tile_set, tile_cols, owners, live_flags = tile_store
    vector_table = vector_bf.reshape(-1, tile_set.shape[2])
    column_hot = (
        tile_cols[:, None] == jnp.arange(vector_table.shape[0], dtype=jnp.int32)[None, :]
    ).astype(jnp.bfloat16)
    picked = jnp.dot(column_hot, vector_table, preferred_element_type=jnp.float32).astype(
        jnp.bfloat16
    )
    product = jnp.einsum("src,sc->sr", tile_set, picked, preferred_element_type=jnp.float32)
    product = jnp.where(live_flags[:, None], product, 0.0)
    owner_hot = (jnp.arange(blocks, dtype=jnp.int32)[:, None] == owners[None, :]).astype(
        jnp.float32
    )
    return jnp.dot(owner_hot, product, precision=lax.Precision.HIGHEST)


def column_products(tile_store, rows_bf):
    tile_set, tile_cols, owners, live_flags = tile_store
    blocks = rows_bf.shape[0]
    owner_hot = (owners[:, None] == jnp.arange(blocks, dtype=jnp.int32)[None, :]).astype(
        jnp.bfloat16
    )
    picked_rows = jnp.dot(owner_hot, rows_bf, preferred_element_type=jnp.float32).astype(
        jnp.bfloat16
    )
    product = jnp.einsum("src,sr->sc", tile_set, picked_rows, preferred_element_type=jnp.float32)
    product = jnp.where(live_flags[:, None], product, 0.0)
    column_hot = (jnp.arange(NCB, dtype=jnp.int32)[:, None] == tile_cols[None, :]).astype(
        jnp.float32
    )
    return jnp.dot(column_hot, product, precision=lax.Precision.HIGHEST).reshape(-1)


def per_device(
    matrix_tiles,
    tile_column,
    block_counts,
    destination,
    row_bounds,
    dual_start,
    primal_start,
    cost_vector,
    upper_bound,
):
    blocks = block_counts.shape[0]
    rows_per = matrix_tiles.shape[1]
    slot_count = matrix_tiles.shape[0]
    starts = jnp.cumsum(block_counts) - block_counts
    slot_ids = jnp.arange(slot_count, dtype=jnp.int32)
    owners = jnp.sum((starts[None, 1:] <= slot_ids[:, None]).astype(jnp.int32), axis=1)
    bounds_here = row_bounds.reshape(blocks, rows_per)
    dual_here = dual_start.reshape(blocks, rows_per)
    peer_ids = jnp.arange(blocks, dtype=jnp.int32)
    inverse = jnp.sum(
        jnp.where(destination[None, :] == peer_ids[:, None], peer_ids[None, :], 0), axis=1
    )
    tile_store = (matrix_tiles, tile_column, owners, slot_ids < jnp.sum(block_counts))
    bounds = bounds_here.astype(jnp.float32)
    dual_state = dual_here.astype(jnp.float32)
    primal = primal_start
    weight = jnp.ones((), jnp.float32)
    row_image = row_products(tile_store, primal.astype(jnp.bfloat16), blocks)
    for iteration in range(ITERS):
        step_primal = step_scale / weight
        step_dual = step_scale * weight
        partial_value = column_products(tile_store, dual_state.astype(jnp.bfloat16))
        gradient = lax.psum(partial_value, ("grp", "dev"))
        primal_next = jnp.clip(primal - step_primal * (cost_vector - gradient), 0.0, upper_bound)
        change = jnp.sum((primal_next - primal) ** 2)
        next_image = row_products(tile_store, primal_next.astype(jnp.bfloat16), blocks)
        dual_state = jnp.maximum(
            dual_state + step_dual * (bounds - (2.0 * next_image - row_image)), 0.0
        )
        violation_part = jnp.sum(jnp.maximum(bounds - next_image, 0.0) ** 2)
        violation = lax.psum(violation_part, ("grp", "dev"))
        weight = jnp.sqrt(weight * jnp.sqrt((violation + 1e-06) / (change + 1e-06)))
        primal = primal_next
        row_image = next_image
    dual_final = lax.all_to_all(
        dual_state[inverse], "dev", split_axis=0, concat_axis=0, tiled=True
    ).reshape(-1)
    return (primal, dual_final, jnp.reshape(weight, (1,)))


MESH_ID = pl.DeviceIdType.MESH
LANES = 128
TILE = 4


def fits(mesh_shape, slots, rows_per, width, blocks, column_blocks):
    n_grp, n_dev = mesh_shape["grp"], mesh_shape["dev"]
    n_chip = n_dev // 2
    if n_dev % 2 or n_chip & (n_chip - 1) or n_grp & (n_grp - 1) or width != n_dev * LANES:
        return False
    if rows_per != LANES or blocks != n_dev or blocks != 8 or slots > 32:
        return False
    if slots % 4 or (n_grp * n_dev * slots) % LANES or column_blocks % LANES:
        return False
    held = slots * rows_per * width * 4 + column_blocks * width * 4 * 5
    return held < 30 * 2**20


def split_kernel(
    n_grp,
    n_dev,
    cols_in,
    counts_in,
    dest_in,
    bounds_in,
    dual_in,
    tiles,
    primal_in,
    cost_in,
    upper_in,
    out_primal,
    out_dual,
    out_weight,
    kv,
    kvt,
    pv,
    cv,
    uv,
    cs,
    us,
    pnow,
    pbf,
    hot,
    hot_back,
    asend,
    abuf,
    bsend,
    bbuf,
    stat,
    dsend,
    drecv,
    cols_at,
    counts_at,
    dest_at,
    bounds_at,
    dual_at,
    tile_sem,
    local_sem,
    small_sem,
    a_send,
    a_recv,
    b_send,
    b_recv,
    stat_send,
    stat_recv,
    f_send,
    f_recv,
    p_send,
    p_recv,
    dual_send,
    dual_recv,
):
    slots, rows_per, width = tiles.shape
    blocks = bounds_in.shape[0]
    n_cb = pnow.shape[0]
    n_all = n_grp * n_dev
    n_chip = n_dev // 2
    span = 2 * LANES
    packs = slots // TILE
    f32, bf16, i32 = jnp.float32, jnp.bfloat16, jnp.int32
    g = lax.axis_index("grp")
    d = lax.axis_index("dev")
    core = d % 2
    chip = d // 2
    twin = 1 - core
    partner = chip * 2 + twin
    me = g * n_dev + d

    def remote(src, dst, ssem, rsem, tg, td):
        return pltpu.make_async_remote_copy(
            src_ref=src,
            dst_ref=dst,
            send_sem=ssem,
            recv_sem=rsem,
            device_id={"grp": tg, "dev": td},
            device_id_type=MESH_ID,
        )

    def bytes_of(ref, ssem, rsem):
        return remote(ref, ref, ssem, rsem, g, partner)

    others = [(a, b) for a in range(n_grp) for b in range(n_dev) if a or b]

    def other(a, b):
        return (g + a) % n_grp, (d + b) % n_dev

    def chunk(u):
        return pl.ds(pl.multiple_of((chip ^ u) * span, span), span)

    barrier = pltpu.get_barrier_semaphore()
    for a, b in others:
        tg, td = other(a, b)
        pl.semaphore_signal(
            barrier, inc=1, device_id={"grp": tg, "dev": td}, device_id_type=MESH_ID
        )
    small = [
        pltpu.make_async_copy(src, dst, small_sem.at[k])
        for k, (src, dst) in enumerate(
            (
                (cols_in, cols_at),
                (counts_in, counts_at),
                (dest_in, dest_at),
                (bounds_in, bounds_at),
                (dual_in, dual_at),
            )
        )
    ]
    for copy in small:
        copy.start()
    order = [u for u in range(n_chip - 1, 0, -1)] + [0]
    planes = sorted(range(1, n_grp), key=lambda a: (-(a.bit_length()), a))
    stages = [[0], [u for u in range(1, n_chip - 1)], [n_chip - 1]]
    part = 4

    def fetch(u):
        for k in range(0, slots, part):
            pltpu.make_async_copy(
                tiles.at[pl.ds(k, part), :, chunk(u)],
                kv.at[pl.ds(k, part), :, chunk(u)],
                tile_sem.at[u],
            ).start()

    fetch(order[0])
    copies = [
        pltpu.make_async_copy(primal_in, pv, local_sem.at[0]),
        pltpu.make_async_copy(cost_in, cv, local_sem.at[1]),
        pltpu.make_async_copy(upper_in, uv, local_sem.at[2]),
    ]

    for copy in small:
        copy.wait()
    for u in order[1:]:
        fetch(u)
    cols = [cols_at[k] for k in range(slots)]
    counts = [counts_at[k] for k in range(blocks)]
    dest = [dest_at[k] for k in range(blocks)]
    starts = [counts[0] * 0]
    for b in range(blocks):
        starts.append(starts[-1] + counts[b])
    total = starts[-1]
    live = [jnp.where(s < total, cols[s], -1) for s in range(slots)]
    lane = lax.broadcasted_iota(i32, (1, LANES), 1)
    turn = (me * slots) % LANES
    place = jnp.where(lane < turn, lane - turn + LANES, lane - turn)
    stat_row = jnp.full((1, LANES), -1.0, f32)
    for s in range(slots):
        stat_row = jnp.where(place == s, live[s].astype(f32), stat_row)
    stat[0, me] = stat_row
    rows = 16
    row = lax.broadcasted_iota(i32, (rows, LANES), 0)
    split = (slots // 2 + 1) // 2 * 2
    lead = split % TILE
    groups = []
    for low, high, base in ((0, split, 0), (split, slots, split - lead)):
        slot = row + base
        owner = jnp.zeros((rows, LANES), i32)
        for b in range(1, blocks):
            owner = owner + jnp.where(slot >= starts[b], 1, 0)
        owner = jnp.where((slot < total) & (slot >= low) & (slot < high), owner, -1)
        groups.append((low, high, slot, owner))
    block_row = lax.broadcasted_iota(i32, (blocks, rows_per), 0)
    slot_row = lax.broadcasted_iota(i32, (slots, rows_per), 0)
    bounds = bounds_at[...].astype(f32)
    dual = dual_at[...].astype(f32)

    def pieces(it, dual_now, before):
        left = {}
        for low, high, slot, owner in groups:
            spread = jnp.zeros((rows, rows_per), f32)
            for b in range(blocks):
                spread = jnp.where(owner == b, dual_now[b : b + 1, :], spread)
            for s in range(low, high, 2):
                left[s] = jnp.concatenate(
                    [jnp.where(slot == s, spread, 0.0), jnp.where(slot == s + 1, spread, 0.0)],
                    axis=1,
                ).astype(bf16)
        for u in order:
            before(u)
            sums = []
            for low, high, _, _ in groups:
                whole = jnp.zeros((rows, span), f32)
                for s in range(low, high, 2):
                    pair = kv[s : s + 2, :, chunk(u)].reshape(2 * rows_per, span)
                    whole = whole + jnp.dot(left[s], pair, preferred_element_type=f32)
                sums.append(whole)
            head, tail = sums[0], sums[1]
            even = split - lead
            joined = [head[:even]]
            if lead:
                joined.append(head[even : even + TILE] + tail[:TILE])
                joined.append(tail[TILE : slots - even])
            else:
                joined.append(tail[: slots - even])
            halves = [
                [
                    x[:, h * LANES : (h + 1) * LANES].astype(bf16).reshape(-1, TILE, LANES)
                    for x in joined
                ]
                for h in range(2)
            ]
            halves = [jnp.concatenate(x, axis=0) for x in halves]
            for h in range(2):
                asend[it, u, h] = halves[h]
            if u == 0:
                abuf[it, pl.ds(me * packs, packs)] = jnp.where(core == 0, halves[0], halves[1])

    def send_pieces(it, u):
        def send(src, tg, td):
            remote(
                src,
                abuf.at[it, pl.ds(me * packs, packs)],
                a_send.at[it],
                a_recv.at[it],
                tg,
                td,
            ).start()

        for a in planes:
            for h in range(2):
                send(asend.at[it, u, h], g ^ a, (chip ^ u) * 2 + h)
        if u:
            for h in range(2):
                send(asend.at[it, u, h], g, (chip ^ u) * 2 + h)
        else:
            send(asend.at[it, 0, twin], g, partner)

    def send_stat(turn_no):
        for a, b in others:
            tg, td = other(a, b)
            remote(
                stat.at[turn_no, me],
                stat.at[turn_no, me],
                stat_send.at[turn_no],
                stat_recv.at[turn_no],
                tg,
                td,
            ).start()

    def stat_bytes(turn_no):
        return bytes_of(
            stat.at[turn_no, pl.ds(0, n_all - 1)], stat_send.at[turn_no], stat_recv.at[turn_no]
        )

    def piece_bytes(it):
        return bytes_of(
            abuf.at[it, pl.ds(0, (n_all - 1) * packs)], a_send.at[it], a_recv.at[it]
        )

    owners = []

    def find_owners():
        for k in range(slots):
            who = jnp.int32(0)
            for b in range(1, blocks):
                who = who + jnp.where(starts[b] <= k, 1, 0)
            owners.append(jnp.where(k < total, who, -1))

    def turn_tiles():
        for s in range(slots):
            at = (s % 2) * rows_per
            for j in range(n_dev):
                kvt[s // 2, j * LANES : (j + 1) * LANES, at : at + rows_per] = kv[
                    s, :, j * LANES : (j + 1) * LANES
                ].T

    def image_part(acc, picks):
        found = jnp.zeros((slots, rows_per), f32)
        for s in range(0, slots, 2):
            out = jnp.zeros((slots, 2 * rows_per), f32)
            for picked, at in picks:
                out = out + jnp.dot(picked, kvt[s // 2, at, :], preferred_element_type=f32)
            found = jnp.where(slot_row == s, out[:, :rows_per], found)
            found = jnp.where(slot_row == s + 1, out[:, rows_per:], found)
        return found if acc is None else acc + found

    def image_of(acc):
        parts = [jnp.zeros((blocks, rows_per), f32) for _ in range(4)]
        for s in range(slots):
            term = jnp.where(block_row == owners[s], acc[s : s + 1, :], 0.0)
            parts[s % 4] = parts[s % 4] + term
        return (parts[0] + parts[1]) + (parts[2] + parts[3])

    def first_image():
        copies[0].wait()
        for j in range(n_dev):
            value = pv[pl.ds(j, n_cb, stride=n_dev), :]
            pbf[:, j * LANES : (j + 1) * LANES] = value.astype(bf16)
        pnow[...] = pv[pl.ds(d, n_cb, stride=n_dev), :]
        wide = lax.broadcasted_iota(i32, (32, n_cb), 0)
        wide_col = jnp.full((32, n_cb), -1, i32)
        for s in range(slots):
            wide_col = jnp.where(wide == s, live[s], wide_col)
        own_hot = jnp.where(
            wide_col == lax.broadcasted_iota(i32, (32, n_cb), 1), 1.0, 0.0
        ).astype(bf16)
        picked = jnp.dot(own_hot, pbf[...], preferred_element_type=f32).astype(bf16)[:slots]
        spans = [slice(c * span, (c + 1) * span) for c in range(n_chip)]
        return image_of(image_part(None, [(picked[:, at], at) for at in spans]))

    def build_hot():
        stat_bytes(0).wait_recv()
        block_of = lax.broadcasted_iota(i32, (n_cb, LANES), 0).astype(f32)
        for t in range(n_all * slots // LANES):
            line = jnp.full((1, LANES), -1.0, f32)
            for k in range(n_all):
                low, high = k * slots - t * LANES, (k + 1) * slots - t * LANES
                if high > 0 and low < LANES:
                    line = jnp.where((lane >= low) & (lane < high), stat[0, k], line)
            hot[:, t * LANES : (t + 1) * LANES] = jnp.where(block_of == line, 1.0, 0.0).astype(bf16)
        back = n_dev * slots
        back_row = lax.broadcasted_iota(i32, (back, LANES), 0)
        back_lane = lax.broadcasted_iota(i32, (back, LANES), 1)
        back_dev, back_slot = back_row // slots, back_row % slots
        found = jnp.zeros((back, LANES), f32)
        for u in range(n_chip):
            for h in range(2):
                src = g * n_dev + (chip ^ u) * 2 + h
                shift = (src * slots) % LANES
                at = jnp.where(back_lane < shift, back_lane - shift + LANES, back_lane - shift)
                hit = (back_dev == u * 2 + h) & (at == back_slot)
                found = jnp.where(hit, stat[0, src] + 1.0, found)
        wanted = jnp.sum(found, axis=1, keepdims=True) - 1.0
        lane_cb = lax.broadcasted_iota(i32, (back, n_cb), 1).astype(f32)
        hot_back[...] = jnp.where(wanted == lane_cb, 1.0, 0.0).astype(bf16)

    def load_slices():
        copies[1].wait()
        copies[2].wait()
        cs[...] = cv[pl.ds(d, n_cb, stride=n_dev), :]
        us[...] = uv[pl.ds(d, n_cb, stride=n_dev), :]

    weight = jnp.ones((1, 1), f32)
    image = None
    for it in range(ITERS):
        if it == 0:

            def ready(u):
                if u == order[-1]:
                    for copy in copies:
                        copy.start()
                pltpu.make_async_copy(
                    tiles.at[:, :, chunk(u)], kv.at[:, :, chunk(u)], tile_sem.at[u]
                ).wait()

            pieces(it, dual, ready)
            pl.semaphore_wait(barrier, len(others))
            send_stat(0)
            for u in order:
                send_pieces(it, u)
            find_owners()
            turn_tiles()
            image = first_image()
            load_slices()
            build_hot()
        else:
            sent_before = []

            def flow(u):
                if sent_before:
                    send_pieces(it, sent_before[-1])
                sent_before.append(u)

            pieces(it, dual, flow)
            send_pieces(it, sent_before[-1])
            stat_bytes(it).wait_recv()
            violation = jnp.sum(stat[it], axis=0)[:, LANES - 1 :]
            change = jnp.sum(stat[it, 0:n_dev], axis=0)[:, :1]
            weight = jnp.sqrt(weight * jnp.sqrt((violation + 1e-06) / (change + 1e-06)))
        tau = step_scale / weight
        piece_bytes(it).wait_recv()
        grad = jnp.dot(
            hot[...],
            abuf.at[it].reshape(n_all * slots, LANES)[...],
            preferred_element_type=f32,
        )
        old = pnow[...]
        new = jnp.minimum(jnp.maximum(old - tau * (cs[...] - grad), 0.0), us[...])
        back = jnp.dot(hot_back[...], new.astype(bf16), preferred_element_type=f32)
        back = back.astype(bf16).reshape(n_chip, 2, packs, TILE, LANES)
        bsend[it] = back
        bbuf[it, 0, core] = jnp.where(core == 0, back[0, 0], back[0, 1])

        def send_back(src, dst, u, td):
            remote(src, dst, b_send.at[it], b_recv.at[it, u], g, td).start()

        for u in order[:-1]:
            for h in range(2):
                send_back(
                    bsend.at[it, u, h], bbuf.at[it, u, core], u, (chip ^ u) * 2 + h
                )
        send_back(bsend.at[it, 0, twin], bbuf.at[it, 0, core], 0, partner)
        gap = new - old
        moved = jnp.sum(gap * gap, axis=(0, 1), keepdims=True)
        if it < ITERS - 1:
            pnow[...] = new
        else:
            out_primal[d] = new
            for u in order[:-1]:
                remote(
                    out_primal.at[d],
                    out_primal.at[d],
                    f_send.at[0],
                    f_recv.at[u],
                    g,
                    (chip ^ u) * 2 + core,
                ).start()
            remote(
                out_primal.at[d], out_primal.at[d], p_send.at[0], p_recv.at[0], g, partner
            ).start()

        acc = None
        for stage in stages:
            picks = []
            for u in stage:
                one = bbuf.at[it, 0, 0] if u == 0 else bbuf.at[it, u]
                bytes_of(one, b_send.at[it], b_recv.at[it, u]).wait_recv()
            for u in stage:
                picked = jnp.concatenate(
                    [bbuf[it, u, h].reshape(slots, LANES) for h in range(2)], axis=1
                )
                picks.append((picked, chunk(u)))
            acc = image_part(acc, picks)
        next_image = image_of(acc)
        sigma = step_scale * weight
        dual = jnp.maximum(dual + sigma * (bounds - (2.0 * next_image - image)), 0.0)
        short = jnp.maximum(bounds - next_image, 0.0)
        image = next_image
        missed = jnp.sum(short * short, axis=(0, 1), keepdims=True)
        stat[it + 1, me] = jnp.where(lane < LANES // 2, moved, missed)
        send_stat(it + 1)

    for e in range(n_dev):
        line = jnp.zeros((1, rows_per), f32)
        for k in range(blocks):
            line = jnp.where(dest[k] == e, dual[k : k + 1, :], line)
        dsend[e] = line
    for k in range(1, n_dev):
        td = (d + k) % n_dev
        remote(dsend.at[td], drecv.at[d], dual_send.at[0], dual_recv.at[0], g, td).start()
    drecv[d] = dsend[d]
    for u in range(1, n_chip):
        src = (chip ^ u) * 2 + core
        bytes_of(out_primal.at[src], f_send.at[0], f_recv.at[u]).wait_recv()
        remote(
            out_primal.at[src], out_primal.at[src], p_send.at[0], p_recv.at[0], g, partner
        ).start()
    bytes_of(drecv.at[pl.ds(0, n_dev - 1)], dual_send.at[0], dual_recv.at[0]).wait_recv()
    out_dual[...] = drecv[...]
    stat_bytes(ITERS).wait_recv()
    violation = jnp.sum(stat[ITERS], axis=0)[:, LANES - 1 :]
    change = jnp.sum(stat[ITERS, 0:n_dev], axis=0)[:, :1]
    weight = jnp.sqrt(weight * jnp.sqrt((violation + 1e-06) / (change + 1e-06)))
    out_weight[...] = jnp.broadcast_to(weight, (1, LANES))
    for it in range(ITERS):
        piece_bytes(it).wait_send()
        bytes_of(
            bbuf.at[it, pl.ds(0, n_chip - 1)], b_send.at[it], b_recv.at[it, 0]
        ).wait_send()
        bytes_of(bbuf.at[it, 0, 0], b_send.at[it], b_recv.at[it, 0]).wait_send()
    for turn_no in range(ITERS + 1):
        stat_bytes(turn_no).wait_send()
    bytes_of(drecv.at[pl.ds(0, n_dev - 1)], dual_send.at[0], dual_recv.at[0]).wait_send()
    bytes_of(out_primal.at[pl.ds(0, n_chip - 1)], f_send.at[0], f_recv.at[0]).wait_send()
    bytes_of(out_primal.at[pl.ds(0, n_chip)], p_send.at[0], p_recv.at[0]).wait_send()
    bytes_of(out_primal.at[pl.ds(0, n_chip)], p_send.at[0], p_recv.at[0]).wait_recv()


def place_kernel(slices, dual, weight, out_primal, out_dual, out_weight, flat, sem):
    n_dev, n_cb, _ = slices.shape
    copies = [
        pltpu.make_async_copy(dual, out_dual, sem.at[4]),
        pltpu.make_async_copy(weight, out_weight, sem.at[5]),
    ]
    for copy in copies:
        copy.start()
    part = n_cb // 4
    for q in range(4):
        for j in range(n_dev):
            flat[pl.ds(q * part * n_dev + j, part, stride=n_dev), :] = slices[
                j, q * part : (q + 1) * part, :
            ]
        here = pl.ds(q * part * n_dev, part * n_dev)
        copy = pltpu.make_async_copy(flat.at[here], out_primal.at[here], sem.at[q])
        copy.start()
        copies.append(copy)
    for copy in copies:
        copy.wait()


def split_device(mesh_shape, *args):
    tiles, cols, counts, dest, row_bounds, dual_start, primal, cost, upper = args
    slots, rows_per, width = tiles.shape
    blocks = counts.shape[0]
    n_cb = primal.shape[0] // width
    if not fits(mesh_shape, slots, rows_per, width, blocks, n_cb):
        return per_device(*args)
    n_grp, n_dev = mesh_shape["grp"], mesh_shape["dev"]
    n_all, n_chip = n_grp * n_dev, n_dev // 2
    packs = slots // TILE
    flat = (primal.shape[0] // LANES, LANES)
    f32, bf16 = jnp.float32, jnp.bfloat16
    vmem = pl.BlockSpec(memory_space=pltpu.VMEM)
    far = pl.BlockSpec(memory_space=pltpu.HBM)
    dma = pltpu.SemaphoreType.DMA
    out_primal, out_dual, out_weight = pl.pallas_call(
        functools.partial(split_kernel, n_grp, n_dev),
        name="pdhg_split",
        out_shape=(
            pltpu.VMEM((n_dev, n_cb, LANES), f32),
            pltpu.VMEM((n_dev, 1, rows_per), f32),
            pltpu.VMEM((1, LANES), f32),
        ),
        in_specs=[far] * 9,
        out_specs=(vmem, vmem, vmem),
        scratch_shapes=[
            pltpu.VMEM((slots, rows_per, width), bf16),
            pltpu.VMEM((slots // 2, width, 2 * rows_per), bf16),
            pltpu.VMEM(flat, f32),
            pltpu.VMEM(flat, f32),
            pltpu.VMEM(flat, f32),
            pltpu.VMEM((n_cb, LANES), f32),
            pltpu.VMEM((n_cb, LANES), f32),
            pltpu.VMEM((n_cb, LANES), f32),
            pltpu.VMEM((n_cb, width), bf16),
            pltpu.VMEM((n_cb, n_all * slots), bf16),
            pltpu.VMEM((n_dev * slots, n_cb), bf16),
            pltpu.VMEM((ITERS, n_chip, 2, packs, TILE, LANES), bf16),
            pltpu.VMEM((ITERS, n_all * packs, TILE, LANES), bf16),
            pltpu.VMEM((ITERS, n_chip, 2, packs, TILE, LANES), bf16),
            pltpu.VMEM((ITERS, n_chip, 2, packs, TILE, LANES), bf16),
            pltpu.VMEM((ITERS + 1, n_all, 1, LANES), f32),
            pltpu.VMEM((n_dev, 1, rows_per), f32),
            pltpu.VMEM((n_dev, 1, rows_per), f32),
            pltpu.SMEM((slots,), jnp.int32),
            pltpu.SMEM((blocks,), jnp.int32),
            pltpu.SMEM((blocks,), jnp.int32),
            pltpu.VMEM((blocks, rows_per), bf16),
            pltpu.VMEM((blocks, rows_per), bf16),
            dma((n_chip,)),
            dma((3,)),
            dma((5,)),
            dma((ITERS,)),
            dma((ITERS,)),
            dma((ITERS,)),
            dma((ITERS, n_chip)),
            dma((ITERS + 1,)),
            dma((ITERS + 1,)),
            dma((1,)),
            dma((n_chip,)),
            dma((1,)),
            dma((1,)),
            dma((1,)),
            dma((1,)),
        ],
        compiler_params=pltpu.CompilerParams(
            collective_id=0, has_side_effects=True, vmem_limit_bytes=65 * 10**6
        ),
    )(
        *(
            pltpu.with_memory_space_constraint(x, pltpu.HBM)
            for x in (
                cols,
                counts,
                dest,
                row_bounds.reshape(blocks, rows_per),
                dual_start.reshape(blocks, rows_per),
                tiles,
                primal.reshape(flat),
                cost.reshape(flat),
                upper.reshape(flat),
            )
        )
    )
    primal_final, dual_final, weight_final = pl.pallas_call(
        place_kernel,
        name="pdhg_place",
        out_shape=(
            jax.ShapeDtypeStruct(flat, f32),
            jax.ShapeDtypeStruct((n_dev, 1, rows_per), f32),
            jax.ShapeDtypeStruct((1, LANES), f32),
        ),
        in_specs=[vmem] * 3,
        out_specs=(far, far, far),
        scratch_shapes=[pltpu.VMEM(flat, f32), dma((6,))],
        compiler_params=pltpu.CompilerParams(vmem_limit_bytes=8 * 10**6),
    )(*(pltpu.with_memory_space_constraint(x, pltpu.VMEM) for x in (out_primal, out_dual, out_weight)))
    return primal_final.reshape(-1), dual_final.reshape(-1), weight_final[0, :1]


def solution(mesh):
    in_specs = (
        P(("grp", "dev"), None, None),
        P(("grp", "dev")),
        P(("grp", "dev")),
        P(("grp", "dev")),
        P(("grp", "dev")),
        P(("grp", "dev")),
        P(),
        P(),
        P(),
    )
    out_specs = (P(), P(("grp", "dev")), P())
    return jax.shard_map(
        functools.partial(split_device, dict(mesh.shape)),
        mesh=mesh,
        in_specs=in_specs,
        out_specs=out_specs,
        check_vma=False,
    )
```

```python
import functools

import jax
import jax.numpy as jnp
from jax import lax
from jax.experimental import pallas as pl
from jax.experimental.pallas import tpu as pltpu
from jax.sharding import PartitionSpec as P

NCB = 256
ITERS = 3


step_scale = 0.3


def row_products(tile_store, vector_bf, blocks):
    tile_set, tile_cols, owners, live_flags = tile_store
    vector_table = vector_bf.reshape(-1, tile_set.shape[2])
    column_hot = (
        tile_cols[:, None] == jnp.arange(vector_table.shape[0], dtype=jnp.int32)[None, :]
    ).astype(jnp.bfloat16)
    picked = jnp.dot(column_hot, vector_table, preferred_element_type=jnp.float32).astype(
        jnp.bfloat16
    )
    product = jnp.einsum("src,sc->sr", tile_set, picked, preferred_element_type=jnp.float32)
    product = jnp.where(live_flags[:, None], product, 0.0)
    owner_hot = (jnp.arange(blocks, dtype=jnp.int32)[:, None] == owners[None, :]).astype(
        jnp.float32
    )
    return jnp.dot(owner_hot, product, precision=lax.Precision.HIGHEST)


def column_products(tile_store, rows_bf):
    tile_set, tile_cols, owners, live_flags = tile_store
    blocks = rows_bf.shape[0]
    owner_hot = (owners[:, None] == jnp.arange(blocks, dtype=jnp.int32)[None, :]).astype(
        jnp.bfloat16
    )
    picked_rows = jnp.dot(owner_hot, rows_bf, preferred_element_type=jnp.float32).astype(
        jnp.bfloat16
    )
    product = jnp.einsum("src,sr->sc", tile_set, picked_rows, preferred_element_type=jnp.float32)
    product = jnp.where(live_flags[:, None], product, 0.0)
    column_hot = (jnp.arange(NCB, dtype=jnp.int32)[:, None] == tile_cols[None, :]).astype(
        jnp.float32
    )
    return jnp.dot(column_hot, product, precision=lax.Precision.HIGHEST).reshape(-1)


def per_device(
    matrix_tiles,
    tile_column,
    block_counts,
    destination,
    row_bounds,
    dual_start,
    primal_start,
    cost_vector,
    upper_bound,
):
    blocks = block_counts.shape[0]
    rows_per = matrix_tiles.shape[1]
    slot_count = matrix_tiles.shape[0]
    starts = jnp.cumsum(block_counts) - block_counts
    slot_ids = jnp.arange(slot_count, dtype=jnp.int32)
    owners = jnp.sum((starts[None, 1:] <= slot_ids[:, None]).astype(jnp.int32), axis=1)
    bounds_here = row_bounds.reshape(blocks, rows_per)
    dual_here = dual_start.reshape(blocks, rows_per)
    peer_ids = jnp.arange(blocks, dtype=jnp.int32)
    inverse = jnp.sum(
        jnp.where(destination[None, :] == peer_ids[:, None], peer_ids[None, :], 0), axis=1
    )
    tile_store = (matrix_tiles, tile_column, owners, slot_ids < jnp.sum(block_counts))
    bounds = bounds_here.astype(jnp.float32)
    dual_state = dual_here.astype(jnp.float32)
    primal = primal_start
    weight = jnp.ones((), jnp.float32)
    row_image = row_products(tile_store, primal.astype(jnp.bfloat16), blocks)
    for iteration in range(ITERS):
        step_primal = step_scale / weight
        step_dual = step_scale * weight
        partial_value = column_products(tile_store, dual_state.astype(jnp.bfloat16))
        gradient = lax.psum(partial_value, ("grp", "dev"))
        primal_next = jnp.clip(primal - step_primal * (cost_vector - gradient), 0.0, upper_bound)
        change = jnp.sum((primal_next - primal) ** 2)
        next_image = row_products(tile_store, primal_next.astype(jnp.bfloat16), blocks)
        dual_state = jnp.maximum(
            dual_state + step_dual * (bounds - (2.0 * next_image - row_image)), 0.0
        )
        violation_part = jnp.sum(jnp.maximum(bounds - next_image, 0.0) ** 2)
        violation = lax.psum(violation_part, ("grp", "dev"))
        weight = jnp.sqrt(weight * jnp.sqrt((violation + 1e-06) / (change + 1e-06)))
        primal = primal_next
        row_image = next_image
    dual_final = lax.all_to_all(
        dual_state[inverse], "dev", split_axis=0, concat_axis=0, tiled=True
    ).reshape(-1)
    return (primal, dual_final, jnp.reshape(weight, (1,)))


MESH_ID = pl.DeviceIdType.MESH
LANES = 128
TILE = 4


def fits(mesh_shape, slots, rows_per, width, blocks, column_blocks):
    n_grp, n_dev = mesh_shape["grp"], mesh_shape["dev"]
    n_chip = n_dev // 2
    if n_dev % 2 or n_chip & (n_chip - 1) or n_grp != 4 or width != n_dev * LANES:
        return False
    if rows_per != LANES or blocks != n_dev or blocks != 8 or slots > 32:
        return False
    if slots % 4 or (n_grp * n_dev * slots) % LANES or column_blocks % LANES:
        return False
    held = slots * rows_per * width * 4 + column_blocks * width * 4 * 5
    return held < 30 * 2**20


def split_kernel(
    n_grp,
    n_dev,
    cols_in,
    counts_in,
    dest_in,
    bounds_in,
    dual_in,
    tiles,
    primal_in,
    cost_in,
    upper_in,
    out_primal,
    out_dual,
    out_weight,
    kv,
    kvt,
    pv,
    cv,
    uv,
    cs,
    us,
    pnow,
    pbf,
    hot,
    hot_back,
    asend,
    abuf,
    bsend,
    bbuf,
    stat,
    shift,
    dsend,
    drecv,
    cols_at,
    counts_at,
    dest_at,
    bounds_at,
    dual_at,
    tile_sem,
    local_sem,
    small_sem,
    a_send,
    a_recv,
    b_send,
    b_recv,
    stat_send,
    stat_recv,
    f_send,
    f_recv,
    p_send,
    p_recv,
    n_send,
    n_recv,
    dual_send,
    dual_recv,
):
    slots, rows_per, width = tiles.shape
    blocks = bounds_in.shape[0]
    n_cb = pnow.shape[0]
    n_all = n_grp * n_dev
    n_chip = n_dev // 2
    span = 2 * LANES
    packs = slots // TILE
    f32, bf16, i32 = jnp.float32, jnp.bfloat16, jnp.int32
    g = lax.axis_index("grp")
    d = lax.axis_index("dev")
    core = d % 2
    chip = d // 2
    twin = 1 - core
    partner = chip * 2 + twin
    me = g * n_dev + d
    low_mid = n_grp // 2 - 1
    near = jnp.where(g <= low_mid, low_mid, low_mid + 1)
    away = n_grp - 1 - near
    is_owner = g == near
    beside = g ^ 1

    def remote(src, dst, ssem, rsem, tg, td):
        return pltpu.make_async_remote_copy(
            src_ref=src,
            dst_ref=dst,
            send_sem=ssem,
            recv_sem=rsem,
            device_id={"grp": tg, "dev": td},
            device_id_type=MESH_ID,
        )

    def bytes_of(ref, ssem, rsem):
        return remote(ref, ref, ssem, rsem, g, partner)

    others = [(a, b) for a in range(n_grp) for b in range(n_dev) if a or b]

    def other(a, b):
        return (g + a) % n_grp, (d + b) % n_dev

    def chunk(u):
        return pl.ds(pl.multiple_of((chip ^ u) * span, span), span)

    barrier = pltpu.get_barrier_semaphore()
    for a, b in others:
        tg, td = other(a, b)
        pl.semaphore_signal(
            barrier, inc=1, device_id={"grp": tg, "dev": td}, device_id_type=MESH_ID
        )
    small = [
        pltpu.make_async_copy(src, dst, small_sem.at[k])
        for k, (src, dst) in enumerate(
            (
                (cols_in, cols_at),
                (counts_in, counts_at),
                (dest_in, dest_at),
                (bounds_in, bounds_at),
                (dual_in, dual_at),
            )
        )
    ]
    for copy in small:
        copy.start()
    order = [u for u in range(n_chip - 1, 0, -1)] + [0]
    planes = sorted(range(1, n_grp), key=lambda a: (-(a.bit_length()), a))
    wide = ITERS - 1
    stages = [[0], [u for u in range(1, n_chip - 1)], [n_chip - 1]]
    part = 4

    def fetch(u):
        for k in range(0, slots, part):
            pltpu.make_async_copy(
                tiles.at[pl.ds(k, part), :, chunk(u)],
                kv.at[pl.ds(k, part), :, chunk(u)],
                tile_sem.at[u],
            ).start()

    fetch(order[0])
    copies = [
        pltpu.make_async_copy(primal_in, pv, local_sem.at[0]),
        pltpu.make_async_copy(cost_in, cv, local_sem.at[1]),
        pltpu.make_async_copy(upper_in, uv, local_sem.at[2]),
    ]

    for copy in small:
        copy.wait()
    for u in order[1:]:
        fetch(u)
    cols = [cols_at[k] for k in range(slots)]
    counts = [counts_at[k] for k in range(blocks)]
    dest = [dest_at[k] for k in range(blocks)]
    starts = [counts[0] * 0]
    for b in range(blocks):
        starts.append(starts[-1] + counts[b])
    total = starts[-1]
    live = [jnp.where(s < total, cols[s], -1) for s in range(slots)]
    lane = lax.broadcasted_iota(i32, (1, LANES), 1)
    turn = (me * slots) % LANES
    place = jnp.where(lane < turn, lane - turn + LANES, lane - turn)
    stat_row = jnp.full((1, LANES), -1.0, f32)
    for s in range(slots):
        stat_row = jnp.where(place == s, live[s].astype(f32), stat_row)
    stat[0, me] = stat_row
    rows = 16
    row = lax.broadcasted_iota(i32, (rows, LANES), 0)
    split = (slots // 2 + 1) // 2 * 2
    lead = split % TILE
    groups = []
    for low, high, base in ((0, split, 0), (split, slots, split - lead)):
        slot = row + base
        owner = jnp.zeros((rows, LANES), i32)
        for b in range(1, blocks):
            owner = owner + jnp.where(slot >= starts[b], 1, 0)
        owner = jnp.where((slot < total) & (slot >= low) & (slot < high), owner, -1)
        groups.append((low, high, slot, owner))
    block_row = lax.broadcasted_iota(i32, (blocks, rows_per), 0)
    slot_row = lax.broadcasted_iota(i32, (slots, rows_per), 0)
    bounds = bounds_at[...].astype(f32)
    dual = dual_at[...].astype(f32)

    def pieces(it, dual_now, before):
        left = {}
        for low, high, slot, owner in groups:
            spread = jnp.zeros((rows, rows_per), f32)
            for b in range(blocks):
                spread = jnp.where(owner == b, dual_now[b : b + 1, :], spread)
            for s in range(low, high, 2):
                left[s] = jnp.concatenate(
                    [jnp.where(slot == s, spread, 0.0), jnp.where(slot == s + 1, spread, 0.0)],
                    axis=1,
                ).astype(bf16)
        for u in order:
            before(u)
            sums = []
            for low, high, _, _ in groups:
                whole = jnp.zeros((rows, span), f32)
                for s in range(low, high, 2):
                    pair = kv[s : s + 2, :, chunk(u)].reshape(2 * rows_per, span)
                    whole = whole + jnp.dot(left[s], pair, preferred_element_type=f32)
                sums.append(whole)
            head, tail = sums[0], sums[1]
            even = split - lead
            joined = [head[:even]]
            if lead:
                joined.append(head[even : even + TILE] + tail[:TILE])
                joined.append(tail[TILE : slots - even])
            else:
                joined.append(tail[: slots - even])
            halves = [
                [
                    x[:, h * LANES : (h + 1) * LANES].astype(bf16).reshape(-1, TILE, LANES)
                    for x in joined
                ]
                for h in range(2)
            ]
            halves = [jnp.concatenate(x, axis=0) for x in halves]
            for h in range(2):
                asend[it, u, h] = halves[h]
            if u == 0:
                abuf[it, pl.ds(me * packs, packs)] = jnp.where(core == 0, halves[0], halves[1])

    def send_pieces(it, u):
        def send(src, tg, td):
            remote(
                src,
                abuf.at[it, pl.ds(me * packs, packs)],
                a_send.at[it],
                a_recv.at[it],
                tg,
                td,
            ).start()

        if it < wide:
            for h in range(2):
                send(asend.at[it, u, h], away, (chip ^ u) * 2 + h)
            if u:
                for h in range(2):
                    send(asend.at[it, u, h], near, (chip ^ u) * 2 + h)
            else:
                send(asend.at[it, 0, twin], near, partner)

                @pl.when(jnp.logical_not(is_owner))
                def _():
                    send(asend.at[it, 0, core], near, d)

            return
        for a in planes:
            for h in range(2):
                send(asend.at[it, u, h], g ^ a, (chip ^ u) * 2 + h)
        if u:
            for h in range(2):
                send(asend.at[it, u, h], g, (chip ^ u) * 2 + h)
        else:
            send(asend.at[it, 0, twin], g, partner)

    def send_stat(turn_no):
        for a, b in others:
            tg, td = other(a, b)
            remote(
                stat.at[turn_no, me],
                stat.at[turn_no, me],
                stat_send.at[turn_no],
                stat_recv.at[turn_no],
                tg,
                td,
            ).start()

    def stat_bytes(turn_no):
        return bytes_of(
            stat.at[turn_no, pl.ds(0, n_all - 1)], stat_send.at[turn_no], stat_recv.at[turn_no]
        )

    def piece_bytes(it):
        return bytes_of(
            abuf.at[it, pl.ds(0, (n_all - 1) * packs)], a_send.at[it], a_recv.at[it]
        )

    owners = []

    def find_owners():
        for k in range(slots):
            who = jnp.int32(0)
            for b in range(1, blocks):
                who = who + jnp.where(starts[b] <= k, 1, 0)
            owners.append(jnp.where(k < total, who, -1))

    def back_sent(it):
        most = bbuf.at[it, pl.ds(0, n_chip - 1)]
        bytes_of(most, b_send.at[it], b_recv.at[it, 0]).wait_send()
        bytes_of(bbuf.at[it, 0, 0], b_send.at[it], b_recv.at[it, 0]).wait_send()

    def turn_tiles():
        for s in range(slots):
            at = (s % 2) * rows_per
            for j in range(n_dev):
                kvt[s // 2, j * LANES : (j + 1) * LANES, at : at + rows_per] = kv[
                    s, :, j * LANES : (j + 1) * LANES
                ].T

    def image_part(acc, picks):
        found = jnp.zeros((slots, rows_per), f32)
        for s in range(0, slots, 2):
            out = jnp.zeros((slots, 2 * rows_per), f32)
            for picked, at in picks:
                out = out + jnp.dot(picked, kvt[s // 2, at, :], preferred_element_type=f32)
            found = jnp.where(slot_row == s, out[:, :rows_per], found)
            found = jnp.where(slot_row == s + 1, out[:, rows_per:], found)
        return found if acc is None else acc + found

    def image_of(acc):
        parts = [jnp.zeros((blocks, rows_per), f32) for _ in range(4)]
        for s in range(slots):
            term = jnp.where(block_row == owners[s], acc[s : s + 1, :], 0.0)
            parts[s % 4] = parts[s % 4] + term
        return (parts[0] + parts[1]) + (parts[2] + parts[3])

    def first_image():
        copies[0].wait()
        for j in range(n_dev):
            value = pv[pl.ds(j, n_cb, stride=n_dev), :]
            pbf[:, j * LANES : (j + 1) * LANES] = value.astype(bf16)

        @pl.when(is_owner)
        def _():
            pnow[...] = pv[pl.ds(d, n_cb, stride=n_dev), :]

        wide = lax.broadcasted_iota(i32, (32, n_cb), 0)
        wide_col = jnp.full((32, n_cb), -1, i32)
        for s in range(slots):
            wide_col = jnp.where(wide == s, live[s], wide_col)
        own_hot = jnp.where(
            wide_col == lax.broadcasted_iota(i32, (32, n_cb), 1), 1.0, 0.0
        ).astype(bf16)
        picked = jnp.dot(own_hot, pbf[...], preferred_element_type=f32).astype(bf16)[:slots]
        spans = [slice(c * span, (c + 1) * span) for c in range(n_chip)]
        return image_of(image_part(None, [(picked[:, at], at) for at in spans]))

    def build_hot():
        stat_bytes(0).wait_recv()
        block_of = lax.broadcasted_iota(i32, (n_cb, LANES), 0).astype(f32)
        for t in range(n_all * slots // LANES):
            line = jnp.full((1, LANES), -1.0, f32)
            for k in range(n_all):
                low, high = k * slots - t * LANES, (k + 1) * slots - t * LANES
                if high > 0 and low < LANES:
                    line = jnp.where((lane >= low) & (lane < high), stat[0, k], line)
            hot[:, t * LANES : (t + 1) * LANES] = jnp.where(block_of == line, 1.0, 0.0).astype(bf16)
        back = 2 * n_dev * slots
        back_row = lax.broadcasted_iota(i32, (back, LANES), 0)
        back_lane = lax.broadcasted_iota(i32, (back, LANES), 1)
        back_dev, back_slot = back_row // slots, back_row % slots
        found = jnp.zeros((back, LANES), f32)
        for w in range(2):
            for u in range(n_chip):
                for h in range(2):
                    src = (g ^ w) * n_dev + (chip ^ u) * 2 + h
                    turned = (src * slots) % LANES
                    at = back_lane - turned
                    at = jnp.where(at < 0, at + LANES, at)
                    hit = (back_dev == w * n_dev + u * 2 + h) & (at == back_slot)
                    found = jnp.where(hit, stat[0, src] + 1.0, found)
        wanted = jnp.sum(found, axis=1, keepdims=True) - 1.0
        lane_cb = lax.broadcasted_iota(i32, (back, n_cb), 1).astype(f32)
        hot_back[...] = jnp.where(wanted == lane_cb, 1.0, 0.0).astype(bf16)

    def load_slices():
        copies[1].wait()
        copies[2].wait()
        cs[...] = cv[pl.ds(d, n_cb, stride=n_dev), :]
        us[...] = uv[pl.ds(d, n_cb, stride=n_dev), :]

    weight = jnp.ones((1, 1), f32)
    shift[...] = jnp.zeros((1, LANES), f32)
    moved_rows = slice(low_mid * n_dev, (low_mid + 1) * n_dev)
    image = None
    for it in range(ITERS):
        if it == 0:

            def ready(u):
                if u == order[-1]:
                    for copy in copies:
                        copy.start()
                pltpu.make_async_copy(
                    tiles.at[:, :, chunk(u)], kv.at[:, :, chunk(u)], tile_sem.at[u]
                ).wait()

            pieces(it, dual, ready)
            pl.semaphore_wait(barrier, len(others))
            send_stat(0)
            for u in order:
                send_pieces(it, u)
            find_owners()
            turn_tiles()
            image = first_image()
            load_slices()
            build_hot()
        else:
            sent_before = []

            def flow(u):
                if sent_before:
                    send_pieces(it, sent_before[-1])
                sent_before.append(u)

            pieces(it, dual, flow)
            send_pieces(it, sent_before[-1])
            stat_bytes(it).wait_recv()
            violation = jnp.sum(stat[it], axis=0)[:, LANES - 1 :]
            change = jnp.sum(stat[it, moved_rows], axis=0)[:, :1]
            weight = jnp.sqrt(weight * jnp.sqrt((violation + 1e-06) / (change + 1e-06)))
        tau = step_scale / weight
        def step():
            grad = jnp.dot(
                hot[...],
                abuf.at[it].reshape(n_all * slots, LANES)[...],
                preferred_element_type=f32,
            )
            old = pnow[...]
            new = jnp.minimum(jnp.maximum(old - tau * (cs[...] - grad), 0.0), us[...])
            rounded = new.astype(bf16)
            for w in (1, 0) if it < wide else (0,):
                rows_here = slice(w * n_dev * slots, (w + 1) * n_dev * slots)
                back = jnp.dot(hot_back[rows_here], rounded, preferred_element_type=f32)
                back = back.astype(bf16).reshape(n_chip, 2, packs, TILE, LANES)
                bsend[it, w] = back
                if w == 0:
                    bbuf[it, 0, core] = jnp.where(core == 0, back[0, 0], back[0, 1])
                for u in order:
                    for h in range(2):
                        if w or u:
                            send_back(w, u, h, (chip ^ u) * 2 + h)
                if w == 0:
                    send_back(0, 0, twin, partner)
            gap = new - old
            moved = jnp.sum(gap * gap, axis=(0, 1), keepdims=True)
            shift[...] = jnp.broadcast_to(moved, (1, LANES))
            return new

        def send_back(w, u, h, td):
            remote(
                bsend.at[it, w, u, h],
                bbuf.at[it, u, core],
                b_send.at[it],
                b_recv.at[it, u],
                g ^ w,
                td,
            ).start()

        if it < wide:

            @pl.when(is_owner)
            def _():
                piece_bytes(it).wait_recv()
                pnow[...] = step()

        else:
            piece_bytes(it).wait_recv()

            @pl.when(jnp.logical_not(is_owner))
            def _():
                bytes_of(pnow, n_send.at[0], n_recv.at[0]).wait_recv()

            out_primal[d] = step()
            for u in order[:-1]:
                remote(
                    out_primal.at[d],
                    out_primal.at[d],
                    f_send.at[0],
                    f_recv.at[u],
                    g,
                    (chip ^ u) * 2 + core,
                ).start()
            remote(
                out_primal.at[d], out_primal.at[d], p_send.at[0], p_recv.at[0], g, partner
            ).start()

        acc = None
        for stage in stages:
            picks = []
            for u in stage:
                if u == 0 and it < wide:

                    @pl.when(is_owner)
                    def _():
                        bytes_of(bbuf.at[it, 0, 0], b_send.at[it], b_recv.at[it, 0]).wait_recv()

                    @pl.when(jnp.logical_not(is_owner))
                    def _():
                        bytes_of(bbuf.at[it, 0], b_send.at[it], b_recv.at[it, 0]).wait_recv()

                else:
                    one = bbuf.at[it, u] if u else bbuf.at[it, 0, 0]
                    bytes_of(one, b_send.at[it], b_recv.at[it, u]).wait_recv()
            for u in stage:
                picked = jnp.concatenate(
                    [bbuf[it, u, h].reshape(slots, LANES) for h in range(2)], axis=1
                )
                picks.append((picked, chunk(u)))
            acc = image_part(acc, picks)
            if it == wide - 1 and stage == stages[0]:

                @pl.when(is_owner)
                def _():
                    remote(pnow, pnow, n_send.at[0], n_recv.at[0], beside, d).start()

        next_image = image_of(acc)
        sigma = step_scale * weight
        dual = jnp.maximum(dual + sigma * (bounds - (2.0 * next_image - image)), 0.0)
        short = jnp.maximum(bounds - next_image, 0.0)
        image = next_image
        missed = jnp.sum(short * short, axis=(0, 1), keepdims=True)
        stat[it + 1, me] = jnp.where(lane < LANES // 2, shift[...], missed)
        send_stat(it + 1)

    for e in range(n_dev):
        line = jnp.zeros((1, rows_per), f32)
        for k in range(blocks):
            line = jnp.where(dest[k] == e, dual[k : k + 1, :], line)
        dsend[e] = line
    for k in range(1, n_dev):
        td = (d + k) % n_dev
        remote(dsend.at[td], drecv.at[d], dual_send.at[0], dual_recv.at[0], g, td).start()
    drecv[d] = dsend[d]
    for u in range(1, n_chip):
        src = (chip ^ u) * 2 + core
        bytes_of(out_primal.at[src], f_send.at[0], f_recv.at[u]).wait_recv()
        remote(
            out_primal.at[src], out_primal.at[src], p_send.at[0], p_recv.at[0], g, partner
        ).start()
    bytes_of(drecv.at[pl.ds(0, n_dev - 1)], dual_send.at[0], dual_recv.at[0]).wait_recv()
    out_dual[...] = drecv[...]
    stat_bytes(ITERS).wait_recv()
    violation = jnp.sum(stat[ITERS], axis=0)[:, LANES - 1 :]
    change = jnp.sum(stat[ITERS, moved_rows], axis=0)[:, :1]
    weight = jnp.sqrt(weight * jnp.sqrt((violation + 1e-06) / (change + 1e-06)))
    out_weight[...] = jnp.broadcast_to(weight, (1, LANES))
    for it in range(wide):
        sends = 2 * n_dev - 1
        bytes_of(abuf.at[it, pl.ds(0, sends * packs)], a_send.at[it], a_recv.at[it]).wait_send()

        @pl.when(jnp.logical_not(is_owner))
        def _():
            bytes_of(abuf.at[it, pl.ds(0, packs)], a_send.at[it], a_recv.at[it]).wait_send()

        @pl.when(is_owner)
        def _():
            bytes_of(bsend.at[it, 1], b_send.at[it], b_recv.at[it, 0]).wait_send()
            back_sent(it)

    piece_bytes(wide).wait_send()
    back_sent(wide)

    @pl.when(is_owner)
    def _():
        bytes_of(pnow, n_send.at[0], n_recv.at[0]).wait_send()

    for turn_no in range(ITERS + 1):
        stat_bytes(turn_no).wait_send()
    bytes_of(drecv.at[pl.ds(0, n_dev - 1)], dual_send.at[0], dual_recv.at[0]).wait_send()
    bytes_of(out_primal.at[pl.ds(0, n_chip - 1)], f_send.at[0], f_recv.at[0]).wait_send()
    bytes_of(out_primal.at[pl.ds(0, n_chip)], p_send.at[0], p_recv.at[0]).wait_send()
    bytes_of(out_primal.at[pl.ds(0, n_chip)], p_send.at[0], p_recv.at[0]).wait_recv()


def place_kernel(slices, dual, weight, out_primal, out_dual, out_weight, flat, sem):
    n_dev, n_cb, _ = slices.shape
    copies = [
        pltpu.make_async_copy(dual, out_dual, sem.at[4]),
        pltpu.make_async_copy(weight, out_weight, sem.at[5]),
    ]
    for copy in copies:
        copy.start()
    part = n_cb // 4
    for q in range(4):
        for j in range(n_dev):
            flat[pl.ds(q * part * n_dev + j, part, stride=n_dev), :] = slices[
                j, q * part : (q + 1) * part, :
            ]
        here = pl.ds(q * part * n_dev, part * n_dev)
        copy = pltpu.make_async_copy(flat.at[here], out_primal.at[here], sem.at[q])
        copy.start()
        copies.append(copy)
    for copy in copies:
        copy.wait()


def split_device(mesh_shape, *args):
    tiles, cols, counts, dest, row_bounds, dual_start, primal, cost, upper = args
    slots, rows_per, width = tiles.shape
    blocks = counts.shape[0]
    n_cb = primal.shape[0] // width
    if not fits(mesh_shape, slots, rows_per, width, blocks, n_cb):
        return per_device(*args)
    n_grp, n_dev = mesh_shape["grp"], mesh_shape["dev"]
    n_all, n_chip = n_grp * n_dev, n_dev // 2
    packs = slots // TILE
    flat = (primal.shape[0] // LANES, LANES)
    f32, bf16 = jnp.float32, jnp.bfloat16
    vmem = pl.BlockSpec(memory_space=pltpu.VMEM)
    far = pl.BlockSpec(memory_space=pltpu.HBM)
    dma = pltpu.SemaphoreType.DMA
    out_primal, out_dual, out_weight = pl.pallas_call(
        functools.partial(split_kernel, n_grp, n_dev),
        name="pdhg_split",
        out_shape=(
            pltpu.VMEM((n_dev, n_cb, LANES), f32),
            pltpu.VMEM((n_dev, 1, rows_per), f32),
            pltpu.VMEM((1, LANES), f32),
        ),
        in_specs=[far] * 9,
        out_specs=(vmem, vmem, vmem),
        scratch_shapes=[
            pltpu.VMEM((slots, rows_per, width), bf16),
            pltpu.VMEM((slots // 2, width, 2 * rows_per), bf16),
            pltpu.VMEM(flat, f32),
            pltpu.VMEM(flat, f32),
            pltpu.VMEM(flat, f32),
            pltpu.VMEM((n_cb, LANES), f32),
            pltpu.VMEM((n_cb, LANES), f32),
            pltpu.VMEM((n_cb, LANES), f32),
            pltpu.VMEM((n_cb, width), bf16),
            pltpu.VMEM((n_cb, n_all * slots), bf16),
            pltpu.VMEM((2 * n_dev * slots, n_cb), bf16),
            pltpu.VMEM((ITERS, n_chip, 2, packs, TILE, LANES), bf16),
            pltpu.VMEM((ITERS, n_all * packs, TILE, LANES), bf16),
            pltpu.VMEM((ITERS, 2, n_chip, 2, packs, TILE, LANES), bf16),
            pltpu.VMEM((ITERS, n_chip, 2, packs, TILE, LANES), bf16),
            pltpu.VMEM((ITERS + 1, n_all, 1, LANES), f32),
            pltpu.VMEM((1, LANES), f32),
            pltpu.VMEM((n_dev, 1, rows_per), f32),
            pltpu.VMEM((n_dev, 1, rows_per), f32),
            pltpu.SMEM((slots,), jnp.int32),
            pltpu.SMEM((blocks,), jnp.int32),
            pltpu.SMEM((blocks,), jnp.int32),
            pltpu.VMEM((blocks, rows_per), bf16),
            pltpu.VMEM((blocks, rows_per), bf16),
            dma((n_chip,)),
            dma((3,)),
            dma((5,)),
            dma((ITERS,)),
            dma((ITERS,)),
            dma((ITERS,)),
            dma((ITERS, n_chip)),
            dma((ITERS + 1,)),
            dma((ITERS + 1,)),
            dma((1,)),
            dma((n_chip,)),
            dma((1,)),
            dma((1,)),
            dma((1,)),
            dma((1,)),
            dma((1,)),
            dma((1,)),
        ],
        compiler_params=pltpu.CompilerParams(
            collective_id=0, has_side_effects=True, vmem_limit_bytes=65 * 10**6
        ),
    )(
        *(
            pltpu.with_memory_space_constraint(x, pltpu.HBM)
            for x in (
                cols,
                counts,
                dest,
                row_bounds.reshape(blocks, rows_per),
                dual_start.reshape(blocks, rows_per),
                tiles,
                primal.reshape(flat),
                cost.reshape(flat),
                upper.reshape(flat),
            )
        )
    )
    primal_final, dual_final, weight_final = pl.pallas_call(
        place_kernel,
        name="pdhg_place",
        out_shape=(
            jax.ShapeDtypeStruct(flat, f32),
            jax.ShapeDtypeStruct((n_dev, 1, rows_per), f32),
            jax.ShapeDtypeStruct((1, LANES), f32),
        ),
        in_specs=[vmem] * 3,
        out_specs=(far, far, far),
        scratch_shapes=[pltpu.VMEM(flat, f32), dma((6,))],
        compiler_params=pltpu.CompilerParams(vmem_limit_bytes=8 * 10**6),
    )(*(pltpu.with_memory_space_constraint(x, pltpu.VMEM) for x in (out_primal, out_dual, out_weight)))
    return primal_final.reshape(-1), dual_final.reshape(-1), weight_final[0, :1]


def solution(mesh):
    in_specs = (
        P(("grp", "dev"), None, None),
        P(("grp", "dev")),
        P(("grp", "dev")),
        P(("grp", "dev")),
        P(("grp", "dev")),
        P(("grp", "dev")),
        P(),
        P(),
        P(),
    )
    out_specs = (P(), P(("grp", "dev")), P())
    return jax.shard_map(
        functools.partial(split_device, dict(mesh.shape)),
        mesh=mesh,
        in_specs=in_specs,
        out_specs=out_specs,
        check_vma=False,
    )
```
